64 devices in a mesh: batch: 4 (over x, y), seq: 16 (over z, core).
Axes of the slice: x: 2, y: 2, z: 8, core: 2. Of those that a mesh axis runs over, the one named last changes fastest.
The devices are a block of a 4x4x8 slice.
Arguments:
- msa_act: bfloat16 [512, 256, 256], P(('batch', 'seq')), parts along dimension 0
- msa_mask: int32 [512, 256], P(('batch', 'seq')), parts along dimension 0
- pair_act: bfloat16 [1024, 256, 128], P(('batch', 'seq')), parts along dimension 0
- w_pair_bias: bfloat16 [128, 8], replicated
- w_row_in: bfloat16 [256, 1024], replicated
- w_row_out: bfloat16 [256, 256], replicated
- w_col_in: bfloat16 [256, 576], replicated
- w_col_out: bfloat16 [256, 256], replicated
- w_trans_in: bfloat16 [256, 1024], replicated
- w_trans_out: bfloat16 [1024, 256], replicated
Outputs:
- output: bfloat16 [512, 256, 256], P('batch', 'seq'), parts along dimension 0
There are 4 independent parts. The reference program is written for one: setup_inputs(seed, part) draws one part's arguments, and reference() takes and returns one part's arrays. A program takes and returns all parts, laid end to end along the dimension named above; an argument that names none is the same for every part.
All inputs are finite; a program needn't handle non-finite values.
Results may differ from the reference program's by a relative error of at most 0.0144833.
Values are sent between devices in bfloat16 or wider.
A program may use at most 768 MiB of HBM per device.

```python
import jax
import jax.numpy as jnp
from jax import lax

SEQ_DEV = 8
GROUP_SIZE = 16
NUM_SEQ = 128
RESIDUES = 256
MSA_CH = 256
PAIR_CH = 128
NUM_HEADS = 8
HEAD_DIM = 32

HEAD_CH = NUM_HEADS * HEAD_DIM
COL_CH = 2 * HEAD_CH + 2 * HEAD_DIM
TRANS_CH = 4 * MSA_CH
TILE_BUDGET = 2 ** 22
LN_EPS = 1.0e-5
MASK_BIG = 1.0e9
MEAN_EPS = 1.0e-10


def draw_weight(base_key, fan_in, fan_out, gain):
    normal = jax.random.normal(base_key, (fan_in, fan_out), jnp.float32)
    return (gain * fan_in ** -0.5 * normal).astype(jnp.bfloat16)


def draw_mask(mask_key):
    key_cls, key_start, key_len = jax.random.split(mask_key, 3)
    shard_class = jax.random.randint(key_cls, (GROUP_SIZE,), 1, 5)
    len_cap = jnp.repeat(shard_class * (RESIDUES // 4), SEQ_DEV)
    starts = jax.random.randint(key_start, (NUM_SEQ,), 0, RESIDUES)
    lengths = jax.random.randint(key_len, (NUM_SEQ,), 1, len_cap + 1)
    lengths = jnp.where(jnp.arange(NUM_SEQ) == 0, RESIDUES, lengths)
    offset = (jnp.arange(RESIDUES)[None, :] - starts[:, None]) % RESIDUES
    return (offset < lengths[:, None]).astype(jnp.int32)


def setup_inputs(seed: int = 0, part: int = 0) -> dict:
    part_key = jax.random.fold_in(jax.random.key(seed), part)
    key_mask, key_shared, key_shard, key_noise, key_pair = jax.random.split(part_key, 5)
    weight_keys = jax.random.split(jax.random.key(seed + 1), 7)
    shared = jax.random.normal(key_shared, (1, RESIDUES, MSA_CH), jnp.float32)
    per_shard = jnp.repeat(jax.random.normal(key_shard, (GROUP_SIZE, RESIDUES, MSA_CH), jnp.float32), SEQ_DEV, axis=0)
    noise_part = jax.random.normal(key_noise, (NUM_SEQ, RESIDUES, MSA_CH), jnp.float32)
    msa_act = (0.7 * shared + 0.7 * per_shard + 0.7 * noise_part).astype(jnp.bfloat16)
    pair_act = jax.random.normal(key_pair, (RESIDUES, RESIDUES, PAIR_CH), jnp.float32).astype(jnp.bfloat16)
    return {
        'msa_act': msa_act,
        'msa_mask': draw_mask(key_mask),
        'pair_act': pair_act,
        'w_pair_bias': draw_weight(weight_keys[0], PAIR_CH, NUM_HEADS, 1.5),
        'w_row_in': draw_weight(weight_keys[1], MSA_CH, 4 * HEAD_CH, 1.0),
        'w_row_out': draw_weight(weight_keys[2], HEAD_CH, MSA_CH, 3.0),
        'w_col_in': draw_weight(weight_keys[3], MSA_CH, COL_CH, 1.5),
        'w_col_out': draw_weight(weight_keys[4], HEAD_CH, MSA_CH, 2.0),
        'w_trans_in': draw_weight(weight_keys[5], MSA_CH, TRANS_CH, 1.4),
        'w_trans_out': draw_weight(weight_keys[6], TRANS_CH, MSA_CH, 1.5),
    }


def layer_norm(x_in):
    x_f32 = x_in.astype(jnp.float32)
    mean_val = jnp.mean(x_f32, axis=-1, keepdims=True)
    centered = x_f32 - mean_val
    var_val = jnp.mean(centered * centered, axis=-1, keepdims=True)
    return (centered * lax.rsqrt(var_val + LN_EPS)).astype(jnp.bfloat16)


def linear(x_in, weight):
    flat_out = jnp.dot(x_in.reshape(-1, x_in.shape[-1]), weight, preferred_element_type=jnp.float32)
    return flat_out.reshape(x_in.shape[:-1] + (weight.shape[-1],))


def pick_tile(n_rows, per_row):
    best_tile = 1
    for candidate in range(1, n_rows + 1):
        if n_rows % candidate == 0 and candidate * per_row <= TILE_BUDGET:
            best_tile = candidate
    return best_tile


def to_tiles(big_array, tile_rows):
    return big_array.reshape((big_array.shape[0] // tile_rows, tile_rows) + big_array.shape[1:])


def row_tile(act_tile, mask_tile, bias_hij, w_row_in, w_row_out):
    n_rows = act_tile.shape[0]
    projected = linear(layer_norm(act_tile), w_row_in).astype(jnp.bfloat16).astype(jnp.float32)
    projected = projected.reshape(n_rows, RESIDUES, 4, NUM_HEADS, HEAD_DIM)
    logits = jnp.einsum('sihd,sjhd->shij', projected[:, :, 0], projected[:, :, 1]) * HEAD_DIM ** -0.5
    logits = logits + bias_hij[None] + mask_tile[:, None, None, :]
    attn_probs = jax.nn.softmax(logits, axis=-1).astype(jnp.bfloat16).astype(jnp.float32)
    attended = jnp.einsum('shij,sjhd->sihd', attn_probs, projected[:, :, 2])
    gated_out = (jax.nn.sigmoid(projected[:, :, 3]) * attended).astype(jnp.bfloat16)
    row_update = linear(gated_out.reshape(n_rows, RESIDUES, HEAD_CH), w_row_out)
    return (act_tile.astype(jnp.float32) + row_update).astype(jnp.bfloat16)


def col_project(act_tile, w_col_in):
    n_rows = act_tile.shape[0]
    projected = linear(layer_norm(act_tile), w_col_in).astype(jnp.bfloat16).astype(jnp.float32)
    queries = projected[:, :, :HEAD_CH].reshape(n_rows, RESIDUES, NUM_HEADS, HEAD_DIM)
    col_keys = projected[:, :, HEAD_CH:HEAD_CH + HEAD_DIM]
    col_vals = projected[:, :, HEAD_CH + HEAD_DIM:HEAD_CH + 2 * HEAD_DIM]
    col_gates = projected[:, :, HEAD_CH + 2 * HEAD_DIM:].reshape(n_rows, RESIDUES, NUM_HEADS, HEAD_DIM)
    return queries, col_keys, col_vals, col_gates


def reference(msa_act, msa_mask, pair_act, w_pair_bias, w_row_in, w_row_out, w_col_in, w_col_out, w_trans_in, w_trans_out):
    mask_f32 = msa_mask.astype(jnp.float32)
    mask_bias = MASK_BIG * (mask_f32 - 1.0)
    pair_bias = linear(layer_norm(pair_act), w_pair_bias).astype(jnp.bfloat16)
    bias_hij = jnp.transpose(pair_bias, (2, 0, 1)).astype(jnp.float32)
    tile_rows = pick_tile(NUM_SEQ, NUM_HEADS * RESIDUES * RESIDUES)

    def row_body(packed):
        return row_tile(packed[0], packed[1], bias_hij, w_row_in, w_row_out)

    after_row = lax.map(row_body, (to_tiles(msa_act, tile_rows), to_tiles(mask_bias, tile_rows)))

    def stats_body(packed):
        projected = col_project(packed[0], w_col_in)
        q_part = jnp.einsum('sn,snhd->nhd', packed[1], projected[0])
        return q_part, projected[1], projected[2]

    q_parts, col_keys, col_vals = lax.map(stats_body, (after_row, to_tiles(mask_f32, tile_rows)))
    mask_count = jnp.sum(mask_f32, axis=0)
    q_mean = (jnp.sum(q_parts, axis=0) / (mask_count + MEAN_EPS)[:, None, None]).astype(jnp.bfloat16).astype(jnp.float32)
    col_logits = jnp.einsum('nhd,snd->snh', q_mean, col_keys.reshape(NUM_SEQ, RESIDUES, HEAD_DIM)) * HEAD_DIM ** -0.5
    col_logits = col_logits + mask_bias[:, :, None]
    col_probs = jax.nn.softmax(col_logits, axis=0)
    col_out = jnp.einsum('snh,snd->nhd', col_probs, col_vals.reshape(NUM_SEQ, RESIDUES, HEAD_DIM))

    def final_body(act_tile):
        projected = col_project(act_tile, w_col_in)
        gated_out = (jax.nn.sigmoid(projected[3]) * col_out[None]).astype(jnp.bfloat16)
        col_update = linear(gated_out.reshape(act_tile.shape[0], RESIDUES, HEAD_CH), w_col_out)
        after_col = (act_tile.astype(jnp.float32) + col_update).astype(jnp.bfloat16)
        hidden = jnp.maximum(linear(layer_norm(after_col), w_trans_in), 0.0).astype(jnp.bfloat16)
        return (after_col.astype(jnp.float32) + linear(hidden, w_trans_out)).astype(jnp.bfloat16)

    return lax.map(final_body, after_row).reshape(NUM_SEQ, RESIDUES, MSA_CH)
```

```python
import jax
import jax.numpy as jnp
from jax import lax
from jax.sharding import PartitionSpec as P

LN_EPS = 1.0e-5
MASK_BIG = 1.0e9
MEAN_EPS = 1.0e-10


def layer_norm(x_in):
    x_f32 = x_in.astype(jnp.float32)
    mean_val = jnp.mean(x_f32, axis=-1, keepdims=True)
    centered = x_f32 - mean_val
    var_val = jnp.mean(centered * centered, axis=-1, keepdims=True)
    return (centered * lax.rsqrt(var_val + LN_EPS)).astype(jnp.bfloat16)


def pick_tile(n_rows, per_row):
    budget = 2 ** 22
    best_tile = 1
    for candidate in range(1, n_rows + 1):
        if n_rows % candidate == 0 and candidate * per_row <= budget:
            best_tile = candidate
    return best_tile


def row_attention(value_a7, mask_bias, bias_hij, w_row_in, w_row_out):
    n_seq, n_res, n_chans = value_a7.shape
    n_heads = bias_hij.shape[0]
    head_dim = w_row_out.shape[0] // n_heads
    qk_scale = head_dim ** -0.5
    w_row_split = w_row_in.reshape(n_chans, 4, n_heads, head_dim)
    row_proj = jnp.einsum('snc,cfhd->fsnhd', layer_norm(value_a7), w_row_split, preferred_element_type=jnp.float32).astype(jnp.bfloat16)
    tile_rows = pick_tile(n_seq, n_heads * n_res * n_res)
    n_tiles = n_seq // tile_rows
    tiled_proj = row_proj.reshape(4, n_tiles, tile_rows, n_res, n_heads, head_dim)

    def tile_body(packed):
        q_tile, k_tile, v_tile, m_tile = packed
        logits = jnp.einsum('sihd,sjhd->shij', q_tile, k_tile, preferred_element_type=jnp.float32) * qk_scale
        logits = logits + bias_hij[None] + m_tile[:, None, None, :]
        attn_probs = jax.nn.softmax(logits, axis=-1).astype(jnp.bfloat16)
        return jnp.einsum('shij,sjhd->sihd', attn_probs, v_tile, preferred_element_type=jnp.float32)

    attended = lax.map(tile_body, (tiled_proj[0], tiled_proj[1], tiled_proj[2], mask_bias.reshape(n_tiles, tile_rows, n_res)))
    attended = attended.reshape(n_seq, n_res, n_heads, head_dim)
    gated_row = (jax.nn.sigmoid(row_proj[3].astype(jnp.float32)) * attended).astype(jnp.bfloat16)
    row_update = jnp.einsum('snhd,hdc->snc', gated_row, w_row_out.reshape(n_heads, head_dim, n_chans), preferred_element_type=jnp.float32)
    return (value_a7.astype(jnp.float32) + row_update).astype(jnp.bfloat16)


def column_attention(value_a7, value_a8, w_col_in, w_col_out, n_heads):
    n_seq, n_res, n_chans = value_a7.shape
    head_ch = w_col_out.shape[0]
    head_dim = head_ch // n_heads
    col_proj = jnp.einsum('snc,cf->snf', layer_norm(value_a7), w_col_in, preferred_element_type=jnp.float32).astype(jnp.bfloat16)
    queries = col_proj[:, :, :head_ch].reshape(n_seq, n_res, n_heads, head_dim)
    col_keys = col_proj[:, :, head_ch:head_ch + head_dim]
    col_vals = col_proj[:, :, head_ch + head_dim:head_ch + 2 * head_dim]
    col_gates = col_proj[:, :, head_ch + 2 * head_dim:].reshape(n_seq, n_res, n_heads, head_dim)
    mask_f32 = value_a8.astype(jnp.float32)
    q_sum = jnp.einsum('sn,snhd->nhd', value_a8.astype(jnp.bfloat16), queries, preferred_element_type=jnp.float32)
    mask_count = jnp.sum(mask_f32, axis=0)
    q_mean = (q_sum / (mask_count + MEAN_EPS)[:, None, None]).astype(jnp.bfloat16)
    col_logits = jnp.einsum('nhd,snd->snh', q_mean, col_keys, preferred_element_type=jnp.float32) * head_dim ** -0.5
    col_logits = col_logits + (MASK_BIG * (mask_f32 - 1.0))[:, :, None]
    probs = jax.nn.softmax(col_logits, axis=0)
    col_out = jnp.einsum('snh,snd->nhd', probs, col_vals, preferred_element_type=jnp.float32)
    gated_col = (jax.nn.sigmoid(col_gates.astype(jnp.float32)) * col_out[None]).astype(jnp.bfloat16)
    col_update = jnp.einsum('snhd,hdc->snc', gated_col, w_col_out.reshape(n_heads, head_dim, n_chans), preferred_element_type=jnp.float32)
    return (value_a7.astype(jnp.float32) + col_update).astype(jnp.bfloat16)


def transition(value_a7, w_trans_in, w_trans_out):
    hidden = jnp.einsum('snc,cf->snf', layer_norm(value_a7), w_trans_in, preferred_element_type=jnp.float32)
    hidden = jnp.maximum(hidden, 0.0).astype(jnp.bfloat16)
    trans_update = jnp.einsum('snf,fc->snc', hidden, w_trans_out, preferred_element_type=jnp.float32)
    return (value_a7.astype(jnp.float32) + trans_update).astype(jnp.bfloat16)


def solution(mesh):
    def local_block(value_a7, value_a8, pair_act, w_pair_bias, w_row_in, w_row_out, w_col_in, w_col_out, w_trans_in, w_trans_out):
        n_heads = w_pair_bias.shape[1]
        bias_rows = jnp.einsum('ijc,ch->hij', layer_norm(pair_act), w_pair_bias, preferred_element_type=jnp.float32).astype(jnp.bfloat16)
        bias_full = lax.all_gather(bias_rows, 'seq', axis=1, tiled=True)
        mask_bias = MASK_BIG * (value_a8.astype(jnp.float32) - 1.0)
        after_row = row_attention(value_a7, mask_bias, bias_full, w_row_in, w_row_out)
        after_row = lax.all_to_all(after_row, 'seq', 1, 0, tiled=True)
        mask_cols = lax.all_to_all(value_a8, 'seq', 1, 0, tiled=True)
        after_col = column_attention(after_row, mask_cols, w_col_in, w_col_out, n_heads)
        return transition(after_col, w_trans_in, w_trans_out)

    rows_spec = P(('batch', 'seq'))
    return jax.shard_map(local_block, mesh=mesh, in_specs=(rows_spec, rows_spec, rows_spec, P(), P(), P(), P(), P(), P(), P()), out_specs=P('batch', 'seq'), check_vma=False)
```

```python
import functools

import jax
import jax.numpy as jnp
from jax import lax
from jax.experimental import pallas as pl
from jax.experimental.pallas import tpu as pltpu
from jax.sharding import PartitionSpec as P

MESH = pl.DeviceIdType.MESH
LN_EPS = 1.0e-5
MASK_BIG = 1.0e9
MEAN_EPS = 1.0e-10
LOG2E = 1.4426950408889634
EXCLUDED = -3.0e38
F32 = jnp.float32
BF16 = jnp.bfloat16
NT = (((1,), (1,)), ((), ()))


def layer_norm(x_in):
    x = x_in.astype(F32)
    centered = x - jnp.mean(x, axis=-1, keepdims=True)
    var = jnp.mean(centered * centered, axis=-1, keepdims=True)
    return (centered * lax.rsqrt(var + LN_EPS)).astype(BF16)


def dot(a, b):
    return jnp.dot(a, b, preferred_element_type=F32)


def dot_nt(a, b):
    return lax.dot_general(a, b, NT, preferred_element_type=F32)


def iota(shape, dim):
    return lax.broadcasted_iota(jnp.int32, shape, dim)


def block_kernel(dims, e_hbm, m_hbm, z_hbm, wpb_hbm, wri_hbm, wro_hbm, wci_hbm, wco_hbm, wti_hbm, wto_hbm, out_hbm,
                 e_v, m_v, z_v, wpb_v, wri_v, wro_v, wci_v, wco_v, wti_v, wto_v,
                 bias32, bias_all, q_s, k_s, v_s, g_s, mb_s, hm_s, bias_t, gt_s, e1_send, e1_recv,
                 wc_s, mrow_s, qsum_s, kt_s, vt_s, gc_s, x_s, p3_s, co_s, out_v,
                 in_sem, out_sem, chain_sem, pair_sem, bias_sem, send_sem, recv_sem):
    n_dev, n_seq, n_res, ch, heads = dims
    chips = n_dev // 2
    reach = chips // 2
    blk = n_res // n_dev
    hd = ch // heads
    c2 = hd ** -0.5 * LOG2E
    hrows = heads * blk
    prows = n_seq * blk
    me = lax.axis_index("seq")
    z, c = lax.div(me, 2), lax.rem(me, 2)

    def chip_at(offset):
        return lax.rem(z + offset + chips, chips)

    def slot_of(chip, core):
        return chip * 2 + core

    loads = [(z_hbm, z_v), (wpb_hbm, wpb_v), (e_hbm, e_v), (m_hbm, m_v), (wri_hbm, wri_v), (wro_hbm, wro_v),
             (wci_hbm, wci_v), (wco_hbm, wco_v), (wti_hbm, wti_v), (wto_hbm, wto_v)]
    copies = [pltpu.make_async_copy(src, dst, in_sem.at[n]) for n, (src, dst) in enumerate(loads)]
    for copy in copies:
        copy.start()

    barrier = pltpu.get_barrier_semaphore()
    for d in range(1, n_dev):
        pl.semaphore_signal(barrier, inc=1, device_id={"seq": lax.rem(me + d, n_dev)}, device_id_type=MESH)

    copies[0].wait()
    copies[1].wait()
    wpb_t = wpb_v[...]

    def bias_row(i, carry):
        rows = dot_nt(wpb_t, layer_norm(z_v[i]))
        for n in range(n_res // 128):
            bias32[n, pl.ds(i, heads, stride=blk), :] = rows[:, n * 128:(n + 1) * 128]
        return carry

    lax.fori_loop(0, blk, bias_row, 0, unroll=True)
    bias_all[me, :hrows] = jnp.concatenate([bias32[n] for n in range(n_res // 128)], axis=-1).astype(BF16)
    copies[3].wait()
    m_f32 = m_v[...].astype(F32)
    mb_s[...] = (MASK_BIG * LOG2E) * (m_f32 - 1.0)
    bias_all[me, hrows:] = jnp.concatenate([m_f32, m_f32], axis=0).astype(BF16)
    pl.semaphore_wait(barrier, n_dev - 1)

    def bias_copy(slot, sem, chip, core):
        return pltpu.make_async_remote_copy(
            src_ref=bias_all.at[slot], dst_ref=bias_all.at[slot], send_sem=sem, recv_sem=bias_sem.at[slot],
            device_id={"seq": slot_of(chip, core)}, device_id_type=MESH)

    def up(k):
        return bias_copy(slot_of(chip_at(-k), c), chain_sem.at[0, k], chip_at(1), c)

    def down(k):
        return bias_copy(slot_of(chip_at(k), c), chain_sem.at[1, k], chip_at(-1), c)

    def across(offset, t):
        return bias_copy(slot_of(chip_at(offset), c), pair_sem.at[t], z, 1 - c)

    def bias_wait(offset, core):
        bias_copy(slot_of(chip_at(offset), core), pair_sem.at[0], z, c).wait_recv()

    up(0).start()
    down(0).start()
    across(0, 0).start()

    for h in range(heads):
        hm_s[h] = jnp.where(lax.div(iota((blk, ch), 1), hd) == h, 1.0, 0.0).astype(BF16)
    copies[2].wait()
    copies[4].wait()

    def project(s, carry):
        proj = dot(layer_norm(e_v[s]), wri_v[...]).astype(BF16)
        q_s[s] = proj[:, :ch]
        k_s[s] = proj[:, ch:2 * ch]
        v_s[s] = proj[:, 2 * ch:3 * ch]
        g_s[s] = proj[:, 3 * ch:]
        return carry

    lax.fori_loop(0, n_seq, project, 0)
    copies[5].wait()

    lane_head = lax.div(iota((blk, ch), 1), hd)

    def own_head(blocks):
        picked = blocks[0]
        for h in range(1, heads):
            picked = jnp.where(lane_head == h, blocks[h], picked)
        return picked

    def e1_copy(t, core):
        chip = tile_chip(t)
        return pltpu.make_async_remote_copy(
            src_ref=e1_send.at[t, core], dst_ref=e1_recv.at[me], send_sem=send_sem.at[t, core], recv_sem=recv_sem.at[me],
            device_id={"seq": slot_of(chip, core)}, device_id_type=MESH)

    def tile_offset(t):
        k = lax.div(t + 1, 2)
        return k * (1 - 2 * lax.rem(t, 2))

    def tile_chip(t):
        return chip_at(tile_offset(t))

    def row_tile(t, carry):
        k = lax.div(t + 1, 2)

        @pl.when(lax.rem(t, 2) == 1)
        def _():
            bias_wait(-k, c)
            across(-k, t).start()

            @pl.when(k < reach)
            def _():
                up(k).start()
                bias_wait(k, c)
                across(k, t + 1).start()

            @pl.when(k < reach - 1)
            def _():
                down(k).start()

        bias_wait(tile_offset(t), 1 - c)
        chip = tile_chip(t)
        for core in range(2):
            bias_t[core * hrows:(core + 1) * hrows] = bias_all[slot_of(chip, core), :hrows].astype(F32) * LOG2E
        first = pl.multiple_of(chip * (2 * blk), 2 * blk)

        def sequence(s, carry):
            parts = []
            for core in range(2):
                q_rows = q_s[s, pl.ds(first + core * blk, blk), :]
                parts += [q_rows * hm_s[h] for h in range(heads)]
            logits = dot_nt(jnp.concatenate(parts, axis=0), k_s[s])
            mask_row = mb_s[pl.ds(s, 1), :]
            probs = []
            step = hrows // 2
            for r in range(0, 2 * hrows, step):
                x = logits[r:r + step] * c2 + (bias_t[r:r + step] + mask_row)
                p = jnp.exp2(x - jnp.max(x, axis=-1, keepdims=True))
                probs.append((p * (1.0 / jnp.sum(p, axis=-1, keepdims=True))).astype(BF16))
            attended = dot(jnp.concatenate(probs, axis=0), v_s[s])
            for core in range(2):
                o = own_head([attended[core * hrows + h * blk:core * hrows + (h + 1) * blk] for h in range(heads)])
                gate = jax.nn.sigmoid(g_s[s, pl.ds(first + core * blk, blk), :].astype(F32))
                gt_s[core, s] = (gate * o).astype(BF16)
            return carry

        lax.fori_loop(0, n_seq, sequence, 0)
        update = dot(gt_s[...].reshape(2 * prows, ch), wro_v[...])
        for core in range(2):
            e_rows = e_v[:, pl.ds(first + core * blk, blk), :].reshape(prows, ch).astype(F32)
            e1_send[t, core] = (e_rows + update[core * prows:(core + 1) * prows]).astype(BF16)

        @pl.when(t == 0)
        def _():
            e1_recv[me] = e1_send[0, c]
            e1_copy(0, 1 - c).start()

        @pl.when(t > 0)
        def _():
            e1_copy(t, 0).start()
            e1_copy(t, 1).start()

        return carry

    lax.fori_loop(0, chips, row_tile, 0)

    copies[6].wait()
    w_k, w_v = wci_v[ch:ch + hd], wci_v[ch + hd:ch + 2 * hd]
    w_all = jnp.concatenate([wci_v[:ch]] + [w_k] * heads + [w_v] * heads + [wci_v[ch + 2 * hd:]], axis=0)
    eye = jnp.where(iota((ch, ch), 0) == iota((ch, ch), 1), 1.0, 0.0).astype(BF16)
    wc_s[...] = dot_nt(eye, w_all).astype(BF16)

    pad = 2 * n_seq
    m_all = bias_all[:, hrows:, :].reshape(n_dev * pad, n_res)
    pick = jnp.where(iota((n_res, prows), 0) == me * blk + lax.rem(iota((n_res, prows), 1), blk), 1.0, 0.0).astype(BF16)
    m_sel = dot(m_all, pick)
    m_sel = jnp.where(lax.rem(iota((n_dev * pad, prows), 0), pad) == lax.div(iota((n_dev * pad, prows), 1), blk), m_sel, 0.0)
    mrow_s[...] = jnp.sum(m_sel.reshape(n_dev, pad, prows), axis=1)
    same = lax.rem(iota((blk, 2 * prows), 1), blk) == iota((blk, 2 * prows), 0)
    qsum_s[...] = jnp.zeros_like(qsum_s)

    def pair_mask(chip):
        return jnp.concatenate([mrow_s[pl.ds(chip * 2 + core, 1), :] for core in range(2)], axis=1)

    def column_in(t, carry):
        chip = chip_at(-tile_offset(t))

        def arrival(core):
            slot = slot_of(chip, core)
            pltpu.make_async_remote_copy(
                src_ref=e1_send.at[0, 0], dst_ref=e1_recv.at[slot], send_sem=send_sem.at[0, 0], recv_sem=recv_sem.at[slot],
                device_id={"seq": me}, device_id_type=MESH).wait_recv()

        @pl.when(t == 0)
        def _():
            arrival(1 - c)

        @pl.when(t > 0)
        def _():
            arrival(0)
            arrival(1)

        rows = e1_recv[pl.ds(chip * 2, 2)].reshape(2 * prows, ch)
        proj = dot(layer_norm(rows), wc_s[...]).astype(BF16)
        kt_s[chip] = proj[:, ch:2 * ch]
        vt_s[chip] = proj[:, 2 * ch:3 * ch]
        gc_s[chip] = proj[:, 3 * ch:]
        sel = jnp.where(same, pair_mask(chip), 0.0).astype(BF16)
        qsum_s[...] += dot(sel, proj[:, :ch])
        return carry

    lax.fori_loop(0, chips, column_in, 0)

    same1 = same[:, :prows]
    count = jnp.sum(jnp.where(same1, jnp.sum(mrow_s[...], axis=0, keepdims=True), 0.0), axis=-1, keepdims=True)
    q_mean = (qsum_s[...] / (count + MEAN_EPS)).astype(BF16)
    q_rows = jnp.concatenate([q_mean * hm_s[h] for h in range(heads)], axis=0)
    same_h = lax.rem(iota((hrows, 2 * prows), 1), blk) == lax.rem(iota((hrows, 2 * prows), 0), blk)
    top = jnp.full((hrows, 2 * prows), EXCLUDED, F32)
    for chip in range(chips):
        x = dot_nt(q_rows, kt_s[chip]) * c2 + (MASK_BIG * LOG2E) * (pair_mask(chip) - 1.0)
        x = jnp.where(same_h, x, EXCLUDED)
        x_s[chip] = x
        top = jnp.maximum(top, x)
    top = jnp.max(top, axis=-1, keepdims=True)
    total = jnp.zeros((hrows, 2 * prows), F32)
    for chip in range(chips):
        p = jnp.exp2(x_s[chip] - top)
        total = total + p
        for n in range(3):
            piece = p.astype(BF16)
            p3_s[n * hrows:(n + 1) * hrows, chip * 2 * prows:(chip + 1) * 2 * prows] = piece
            p = p - piece.astype(F32)
    o3 = dot(p3_s[...], vt_s[...].reshape(chips * 2 * prows, ch))
    o = (o3[:hrows] + o3[hrows:2 * hrows] + o3[2 * hrows:]) / jnp.sum(total, axis=-1, keepdims=True)
    co_s[...] = own_head([o[h * blk:(h + 1) * blk] for h in range(heads)])

    copies[7].wait()
    copies[8].wait()
    copies[9].wait()

    def finish(chip, carry):
        e1 = e1_recv[pl.ds(chip * 2, 2)].reshape(2 * prows, ch).astype(F32)
        gate = jax.nn.sigmoid(gc_s[chip].astype(F32)).reshape(2 * n_seq, blk, ch)
        gated = (gate * co_s[...][None]).astype(BF16).reshape(2 * prows, ch)
        e2 = (e1 + dot(gated, wco_v[...])).astype(BF16)
        hidden = jnp.maximum(dot(layer_norm(e2), wti_v[...]), 0.0).astype(BF16)
        e3 = (e2.astype(F32) + dot(hidden, wto_v[...])).astype(BF16)
        out_v[pl.ds(chip * 2 * n_seq, 2 * n_seq)] = e3.reshape(2 * n_seq, blk, ch)
        out_copy(chip).start()
        return carry

    def out_copy(chip):
        rows = pl.ds(chip * 2 * n_seq, 2 * n_seq)
        return pltpu.make_async_copy(out_v.at[rows], out_hbm.at[rows], out_sem.at[chip])

    lax.fori_loop(0, chips, finish, 0)

    for k in range(reach):
        up(k).wait_send()
        if k < reach - 1:
            down(k).wait_send()
    for t in range(chips):
        across(0, t).wait_send()
    e1_copy(0, 1 - c).wait_send()
    for t in range(1, chips):
        e1_copy(t, 0).wait_send()
        e1_copy(t, 1).wait_send()
    for chip in range(chips):
        out_copy(chip).wait()


def solution(mesh):
    n_dev = mesh.shape["seq"]

    def local_block(e, m, z, w_pair_bias, w_row_in, w_row_out, w_col_in, w_col_out, w_trans_in, w_trans_out):
        n_seq, n_res, ch = e.shape
        heads = w_pair_bias.shape[1]
        blk = n_res // n_dev
        chips = n_dev // 2
        hrows, prows = heads * blk, n_seq * blk
        args = (e, m, z, w_pair_bias.T, w_row_in, w_row_out, w_col_in.T, w_col_out, w_trans_in, w_trans_out)
        scratch = [pltpu.VMEM(a.shape, a.dtype) for a in args] + [
            pltpu.VMEM((n_res // 128, hrows, 128), F32),
            pltpu.VMEM((n_dev, hrows + 2 * n_seq, n_res), BF16),
            pltpu.VMEM((n_seq, n_res, ch), BF16),
            pltpu.VMEM((n_seq, n_res, ch), BF16),
            pltpu.VMEM((n_seq, n_res, ch), BF16),
            pltpu.VMEM((n_seq, n_res, ch), BF16),
            pltpu.VMEM((n_seq, n_res), F32),
            pltpu.VMEM((heads, blk, ch), BF16),
            pltpu.VMEM((2 * hrows, n_res), F32),
            pltpu.VMEM((2, n_seq, blk, ch), BF16),
            pltpu.VMEM((chips, 2, prows, ch), BF16),
            pltpu.VMEM((n_dev, prows, ch), BF16),
            pltpu.VMEM((ch, 4 * ch), BF16),
            pltpu.VMEM((n_dev, prows), F32),
            pltpu.VMEM((blk, ch), F32),
            pltpu.VMEM((chips, 2 * prows, ch), BF16),
            pltpu.VMEM((chips, 2 * prows, ch), BF16),
            pltpu.VMEM((chips, 2 * prows, ch), BF16),
            pltpu.VMEM((chips, hrows, 2 * prows), F32),
            pltpu.VMEM((3 * hrows, n_dev * prows), BF16),
            pltpu.VMEM((blk, ch), F32),
            pltpu.VMEM((n_dev * n_seq, blk, ch), BF16),
            pltpu.SemaphoreType.DMA((len(args),)),
            pltpu.SemaphoreType.DMA((chips,)),
            pltpu.SemaphoreType.DMA((2, chips // 2)),
            pltpu.SemaphoreType.DMA((chips,)),
            pltpu.SemaphoreType.DMA((n_dev,)),
            pltpu.SemaphoreType.DMA((chips, 2)),
            pltpu.SemaphoreType.DMA((n_dev,)),
        ]
        return pl.pallas_call(
            functools.partial(block_kernel, (n_dev, n_seq, n_res, ch, heads)),
            out_shape=jax.ShapeDtypeStruct((n_dev * n_seq, blk, ch), BF16),
            in_specs=[pl.BlockSpec(memory_space=pl.ANY)] * len(args),
            out_specs=pl.BlockSpec(memory_space=pl.ANY),
            scratch_shapes=scratch,
            name="msa_block",
            compiler_params=pltpu.CompilerParams(collective_id=0, has_side_effects=True, vmem_limit_bytes=60 * 2 ** 20),
        )(*args)

    rows_spec = P(('batch', 'seq'))
    return jax.shard_map(local_block, mesh=mesh, in_specs=(rows_spec, rows_spec, rows_spec, P(), P(), P(), P(), P(), P(), P()), out_specs=P('batch', 'seq'), check_vma=False)
```

```python
import functools

import jax
import jax.numpy as jnp
from jax import lax
from jax.experimental import pallas as pl
from jax.experimental.pallas import tpu as pltpu
from jax.sharding import PartitionSpec as P

MESH = pl.DeviceIdType.MESH
LN_EPS = 1.0e-5
MASK_BIG = 1.0e9
MEAN_EPS = 1.0e-10
LOG2E = 1.4426950408889634
EXCLUDED = -3.0e38
F32 = jnp.float32
BF16 = jnp.bfloat16
NT = (((1,), (1,)), ((), ()))


def layer_norm(x_in):
    x = x_in.astype(F32)
    centered = x - jnp.mean(x, axis=-1, keepdims=True)
    var = jnp.mean(centered * centered, axis=-1, keepdims=True)
    return (centered * lax.rsqrt(var + LN_EPS)).astype(BF16)


def dot(a, b):
    return jnp.dot(a, b, preferred_element_type=F32)


def dot_nt(a, b):
    return lax.dot_general(a, b, NT, preferred_element_type=F32)


def iota(shape, dim):
    return lax.broadcasted_iota(jnp.int32, shape, dim)


def block_kernel(dims, e_hbm, m_hbm, z_hbm, wpb_hbm, wri_hbm, wro_hbm, wci_hbm, wco_hbm, wti_hbm, wto_hbm, out_hbm,
                 e_v, m_v, z_v, wpb_v, wri_v, wro_v, wci_v, wco_v, wti_v, wto_v,
                 bias32, bias_all, q_s, k_s, v_s, g_s, mb_s, hm_s, bias_t, gt_s, e1_send, e1_recv,
                 wc_s, mrow_s, qsum_s, kt_s, vt_s, gc_s, x_s, p3_s, co_s, out_v,
                 in_sem, out_sem, chain_sem, pair_sem, bias_sem, send_sem, recv_sem):
    n_dev, n_seq, n_res, ch, heads = dims
    chips = n_dev // 2
    reach = chips // 2
    blk = n_res // n_dev
    hd = ch // heads
    c2 = hd ** -0.5 * LOG2E
    hrows = heads * blk
    prows = n_seq * blk
    me = lax.axis_index("seq")
    z, c = lax.div(me, 2), lax.rem(me, 2)

    def chip_at(offset):
        return lax.rem(z + offset + chips, chips)

    def slot_of(chip, core):
        return chip * 2 + core

    loads = [(z_hbm, z_v), (wpb_hbm, wpb_v), (e_hbm, e_v), (m_hbm, m_v), (wri_hbm, wri_v), (wro_hbm, wro_v),
             (wci_hbm, wci_v), (wco_hbm, wco_v), (wti_hbm, wti_v), (wto_hbm, wto_v)]
    copies = [pltpu.make_async_copy(src, dst, in_sem.at[n]) for n, (src, dst) in enumerate(loads)]
    for copy in copies:
        copy.start()

    barrier = pltpu.get_barrier_semaphore()
    for d in range(1, n_dev):
        pl.semaphore_signal(barrier, inc=1, device_id={"seq": lax.rem(me + d, n_dev)}, device_id_type=MESH)

    copies[0].wait()
    copies[1].wait()
    wpb_t = wpb_v[...]

    def bias_row(i, carry):
        rows = dot_nt(wpb_t, layer_norm(z_v[i]))
        for n in range(n_res // 128):
            bias32[n, pl.ds(i, heads, stride=blk), :] = rows[:, n * 128:(n + 1) * 128]
        return carry

    lax.fori_loop(0, blk, bias_row, 0, unroll=True)
    bias_all[me, :hrows] = jnp.concatenate([bias32[n] for n in range(n_res // 128)], axis=-1).astype(BF16)
    copies[3].wait()
    m_f32 = m_v[...].astype(F32)
    mb_s[...] = (MASK_BIG * LOG2E) * (m_f32 - 1.0)
    bias_all[me, hrows:] = jnp.concatenate([m_f32, m_f32], axis=0).astype(BF16)
    pl.semaphore_wait(barrier, n_dev - 1)

    def bias_copy(slot, sem, chip, core):
        return pltpu.make_async_remote_copy(
            src_ref=bias_all.at[slot], dst_ref=bias_all.at[slot], send_sem=sem, recv_sem=bias_sem.at[slot],
            device_id={"seq": slot_of(chip, core)}, device_id_type=MESH)

    def up(k):
        return bias_copy(slot_of(chip_at(-k), c), chain_sem.at[0, k], chip_at(1), c)

    def down(k):
        return bias_copy(slot_of(chip_at(k), c), chain_sem.at[1, k], chip_at(-1), c)

    def across(offset, t):
        return bias_copy(slot_of(chip_at(offset), c), pair_sem.at[t], z, 1 - c)

    def bias_wait(offset, core):
        bias_copy(slot_of(chip_at(offset), core), pair_sem.at[0], z, c).wait_recv()

    up(0).start()
    down(0).start()
    across(0, 0).start()

    for h in range(heads):
        hm_s[h] = jnp.where(lax.div(iota((blk, ch), 1), hd) == h, 1.0, 0.0).astype(BF16)
    copies[2].wait()
    copies[4].wait()

    def project(s, carry):
        proj = dot(layer_norm(e_v[s]), wri_v[...]).astype(BF16)
        q_s[s] = proj[:, :ch]
        k_s[s] = proj[:, ch:2 * ch]
        v_s[s] = proj[:, 2 * ch:3 * ch]
        g_s[s] = proj[:, 3 * ch:]
        return carry

    lax.fori_loop(0, n_seq, project, 0, unroll=True)
    copies[5].wait()

    lane_head = lax.div(iota((blk, ch), 1), hd)

    def own_head(blocks):
        picked = blocks[0]
        for h in range(1, heads):
            picked = jnp.where(lane_head == h, blocks[h], picked)
        return picked

    def e1_copy(t, core):
        chip = tile_chip(t)
        return pltpu.make_async_remote_copy(
            src_ref=e1_send.at[t, core], dst_ref=e1_recv.at[me], send_sem=send_sem.at[t, core], recv_sem=recv_sem.at[me],
            device_id={"seq": slot_of(chip, core)}, device_id_type=MESH)

    def tile_offset(t):
        k = lax.div(t + 1, 2)
        return k * (1 - 2 * lax.rem(t, 2))

    def tile_chip(t):
        return chip_at(tile_offset(t))

    def row_tile(t, carry):
        k = lax.div(t + 1, 2)

        @pl.when(lax.rem(t, 2) == 1)
        def _():
            bias_wait(-k, c)
            across(-k, t).start()

            @pl.when(k < reach)
            def _():
                up(k).start()
                bias_wait(k, c)
                across(k, t + 1).start()

            @pl.when(k < reach - 1)
            def _():
                down(k).start()

        bias_wait(tile_offset(t), 1 - c)
        chip = tile_chip(t)
        for core in range(2):
            bias_t[core * hrows:(core + 1) * hrows] = bias_all[slot_of(chip, core), :hrows].astype(F32) * LOG2E
        first = pl.multiple_of(chip * (2 * blk), 2 * blk)

        def logits_of(s):
            parts = []
            for core in range(2):
                q_rows = q_s[s, pl.ds(first + core * blk, blk), :]
                parts += [q_rows * hm_s[h] for h in range(heads)]
            return dot_nt(jnp.concatenate(parts, axis=0), k_s[s])

        logits = logits_of(0)
        for s in range(n_seq):
            ahead = logits_of(s + 1) if s + 1 < n_seq else None
            mask_row = mb_s[s:s + 1, :]
            probs = []
            step = hrows // 2
            for r in range(0, 2 * hrows, step):
                x = logits[r:r + step] * c2 + (bias_t[r:r + step] + mask_row)
                p = jnp.exp2(x - jnp.max(x, axis=-1, keepdims=True))
                probs.append((p * (1.0 / jnp.sum(p, axis=-1, keepdims=True))).astype(BF16))
            attended = dot(jnp.concatenate(probs, axis=0), v_s[s])
            for core in range(2):
                o = own_head([attended[core * hrows + h * blk:core * hrows + (h + 1) * blk] for h in range(heads)])
                gate = jax.nn.sigmoid(g_s[s, pl.ds(first + core * blk, blk), :].astype(F32))
                gt_s[core, s] = (gate * o).astype(BF16)
            logits = ahead
        update = dot(gt_s[...].reshape(2 * prows, ch), wro_v[...])
        for core in range(2):
            e_rows = e_v[:, pl.ds(first + core * blk, blk), :].reshape(prows, ch).astype(F32)
            e1_send[t, core] = (e_rows + update[core * prows:(core + 1) * prows]).astype(BF16)

        @pl.when(t == 0)
        def _():
            e1_recv[me] = e1_send[0, c]
            e1_copy(0, 1 - c).start()

        @pl.when(t > 0)
        def _():
            e1_copy(t, 0).start()
            e1_copy(t, 1).start()

        return carry

    lax.fori_loop(0, chips, row_tile, 0)

    copies[6].wait()
    w_k, w_v = wci_v[ch:ch + hd], wci_v[ch + hd:ch + 2 * hd]
    w_all = jnp.concatenate([wci_v[:ch]] + [w_k] * heads + [w_v] * heads + [wci_v[ch + 2 * hd:]], axis=0)
    eye = jnp.where(iota((ch, ch), 0) == iota((ch, ch), 1), 1.0, 0.0).astype(BF16)
    wc_s[...] = dot_nt(eye, w_all).astype(BF16)

    pad = 2 * n_seq
    m_all = bias_all[:, hrows:, :].reshape(n_dev * pad, n_res)
    pick = jnp.where(iota((n_res, prows), 0) == me * blk + lax.rem(iota((n_res, prows), 1), blk), 1.0, 0.0).astype(BF16)
    m_sel = dot(m_all, pick)
    m_sel = jnp.where(lax.rem(iota((n_dev * pad, prows), 0), pad) == lax.div(iota((n_dev * pad, prows), 1), blk), m_sel, 0.0)
    mrow_s[...] = jnp.sum(m_sel.reshape(n_dev, pad, prows), axis=1)
    same = lax.rem(iota((blk, 2 * prows), 1), blk) == iota((blk, 2 * prows), 0)
    qsum_s[...] = jnp.zeros_like(qsum_s)

    def pair_mask(chip):
        return jnp.concatenate([mrow_s[pl.ds(chip * 2 + core, 1), :] for core in range(2)], axis=1)

    def column_in(t, carry):
        chip = chip_at(-tile_offset(t))

        def arrival(core):
            slot = slot_of(chip, core)
            pltpu.make_async_remote_copy(
                src_ref=e1_send.at[0, 0], dst_ref=e1_recv.at[slot], send_sem=send_sem.at[0, 0], recv_sem=recv_sem.at[slot],
                device_id={"seq": me}, device_id_type=MESH).wait_recv()

        @pl.when(t == 0)
        def _():
            arrival(1 - c)

        @pl.when(t > 0)
        def _():
            arrival(0)
            arrival(1)

        rows = e1_recv[pl.ds(chip * 2, 2)].reshape(2 * prows, ch)
        proj = dot(layer_norm(rows), wc_s[...]).astype(BF16)
        kt_s[chip] = proj[:, ch:2 * ch]
        vt_s[chip] = proj[:, 2 * ch:3 * ch]
        gc_s[chip] = proj[:, 3 * ch:]
        sel = jnp.where(same, pair_mask(chip), 0.0).astype(BF16)
        qsum_s[...] += dot(sel, proj[:, :ch])
        return carry

    lax.fori_loop(0, chips, column_in, 0)

    same1 = same[:, :prows]
    count = jnp.sum(jnp.where(same1, jnp.sum(mrow_s[...], axis=0, keepdims=True), 0.0), axis=-1, keepdims=True)
    q_mean = (qsum_s[...] / (count + MEAN_EPS)).astype(BF16)
    q_rows = jnp.concatenate([q_mean * hm_s[h] for h in range(heads)], axis=0)
    same_h = lax.rem(iota((hrows, 2 * prows), 1), blk) == lax.rem(iota((hrows, 2 * prows), 0), blk)
    top = jnp.full((hrows, 2 * prows), EXCLUDED, F32)
    for chip in range(chips):
        x = dot_nt(q_rows, kt_s[chip]) * c2 + (MASK_BIG * LOG2E) * (pair_mask(chip) - 1.0)
        x = jnp.where(same_h, x, EXCLUDED)
        x_s[chip] = x
        top = jnp.maximum(top, x)
    top = jnp.max(top, axis=-1, keepdims=True)
    total = jnp.zeros((hrows, 2 * prows), F32)
    for chip in range(chips):
        p = jnp.exp2(x_s[chip] - top)
        total = total + p
        for n in range(3):
            piece = p.astype(BF16)
            p3_s[n * hrows:(n + 1) * hrows, chip * 2 * prows:(chip + 1) * 2 * prows] = piece
            p = p - piece.astype(F32)
    o3 = dot(p3_s[...], vt_s[...].reshape(chips * 2 * prows, ch))
    o = (o3[:hrows] + o3[hrows:2 * hrows] + o3[2 * hrows:]) / jnp.sum(total, axis=-1, keepdims=True)
    co_s[...] = own_head([o[h * blk:(h + 1) * blk] for h in range(heads)])

    copies[7].wait()
    copies[8].wait()
    copies[9].wait()

    def finish(pair, carry):
        for n in range(2):
            finish_chip(pair * 2 + n)
        return carry

    def finish_chip(chip):
        e1 = e1_recv[pl.ds(chip * 2, 2)].reshape(2 * prows, ch).astype(F32)
        gate = jax.nn.sigmoid(gc_s[chip].astype(F32)).reshape(2 * n_seq, blk, ch)
        gated = (gate * co_s[...][None]).astype(BF16).reshape(2 * prows, ch)
        e2 = (e1 + dot(gated, wco_v[...])).astype(BF16)
        hidden = jnp.maximum(dot(layer_norm(e2), wti_v[...]), 0.0).astype(BF16)
        e3 = (e2.astype(F32) + dot(hidden, wto_v[...])).astype(BF16)
        out_v[pl.ds(chip * 2 * n_seq, 2 * n_seq)] = e3.reshape(2 * n_seq, blk, ch)
        out_copy(chip).start()

    def out_copy(chip):
        rows = pl.ds(chip * 2 * n_seq, 2 * n_seq)
        return pltpu.make_async_copy(out_v.at[rows], out_hbm.at[rows], out_sem.at[chip])

    lax.fori_loop(0, chips // 2, finish, 0)

    for k in range(reach):
        up(k).wait_send()
        if k < reach - 1:
            down(k).wait_send()
    for t in range(chips):
        across(0, t).wait_send()
    e1_copy(0, 1 - c).wait_send()
    for t in range(1, chips):
        e1_copy(t, 0).wait_send()
        e1_copy(t, 1).wait_send()
    for chip in range(chips):
        out_copy(chip).wait()


def solution(mesh):
    n_dev = mesh.shape["seq"]

    def local_block(e, m, z, w_pair_bias, w_row_in, w_row_out, w_col_in, w_col_out, w_trans_in, w_trans_out):
        n_seq, n_res, ch = e.shape
        heads = w_pair_bias.shape[1]
        blk = n_res // n_dev
        chips = n_dev // 2
        hrows, prows = heads * blk, n_seq * blk
        args = (e, m, z, w_pair_bias.T, w_row_in, w_row_out, w_col_in.T, w_col_out, w_trans_in, w_trans_out)
        scratch = [pltpu.VMEM(a.shape, a.dtype) for a in args] + [
            pltpu.VMEM((n_res // 128, hrows, 128), F32),
            pltpu.VMEM((n_dev, hrows + 2 * n_seq, n_res), BF16),
            pltpu.VMEM((n_seq, n_res, ch), BF16),
            pltpu.VMEM((n_seq, n_res, ch), BF16),
            pltpu.VMEM((n_seq, n_res, ch), BF16),
            pltpu.VMEM((n_seq, n_res, ch), BF16),
            pltpu.VMEM((n_seq, n_res), F32),
            pltpu.VMEM((heads, blk, ch), BF16),
            pltpu.VMEM((2 * hrows, n_res), F32),
            pltpu.VMEM((2, n_seq, blk, ch), BF16),
            pltpu.VMEM((chips, 2, prows, ch), BF16),
            pltpu.VMEM((n_dev, prows, ch), BF16),
            pltpu.VMEM((ch, 4 * ch), BF16),
            pltpu.VMEM((n_dev, prows), F32),
            pltpu.VMEM((blk, ch), F32),
            pltpu.VMEM((chips, 2 * prows, ch), BF16),
            pltpu.VMEM((chips, 2 * prows, ch), BF16),
            pltpu.VMEM((chips, 2 * prows, ch), BF16),
            pltpu.VMEM((chips, hrows, 2 * prows), F32),
            pltpu.VMEM((3 * hrows, n_dev * prows), BF16),
            pltpu.VMEM((blk, ch), F32),
            pltpu.VMEM((n_dev * n_seq, blk, ch), BF16),
            pltpu.SemaphoreType.DMA((len(args),)),
            pltpu.SemaphoreType.DMA((chips,)),
            pltpu.SemaphoreType.DMA((2, chips // 2)),
            pltpu.SemaphoreType.DMA((chips,)),
            pltpu.SemaphoreType.DMA((n_dev,)),
            pltpu.SemaphoreType.DMA((chips, 2)),
            pltpu.SemaphoreType.DMA((n_dev,)),
        ]
        return pl.pallas_call(
            functools.partial(block_kernel, (n_dev, n_seq, n_res, ch, heads)),
            out_shape=jax.ShapeDtypeStruct((n_dev * n_seq, blk, ch), BF16),
            in_specs=[pl.BlockSpec(memory_space=pl.ANY)] * len(args),
            out_specs=pl.BlockSpec(memory_space=pl.ANY),
            scratch_shapes=scratch,
            name="msa_block",
            compiler_params=pltpu.CompilerParams(collective_id=0, has_side_effects=True, vmem_limit_bytes=60 * 2 ** 20),
        )(*args)

    rows_spec = P(('batch', 'seq'))
    return jax.shard_map(local_block, mesh=mesh, in_specs=(rows_spec, rows_spec, rows_spec, P(), P(), P(), P(), P(), P(), P()), out_specs=P('batch', 'seq'), check_vma=False)
```

```python
import functools

import jax
import jax.numpy as jnp
from jax import lax
from jax.experimental import pallas as pl
from jax.experimental.pallas import tpu as pltpu
from jax.sharding import PartitionSpec as P

MESH = pl.DeviceIdType.MESH
LN_EPS = 1.0e-5
MASK_BIG = 1.0e9
MEAN_EPS = 1.0e-10
LOG2E = 1.4426950408889634
EXCLUDED = -3.0e38
F32 = jnp.float32
BF16 = jnp.bfloat16
NT = (((1,), (1,)), ((), ()))


def layer_norm(x_in):
    x = x_in.astype(F32)
    centered = x - jnp.mean(x, axis=-1, keepdims=True)
    var = jnp.mean(centered * centered, axis=-1, keepdims=True)
    return (centered * lax.rsqrt(var + LN_EPS)).astype(BF16)


def dot(a, b):
    return jnp.dot(a, b, preferred_element_type=F32)


def dot_nt(a, b):
    return lax.dot_general(a, b, NT, preferred_element_type=F32)


def iota(shape, dim):
    return lax.broadcasted_iota(jnp.int32, shape, dim)


def block_kernel(dims, e_hbm, m_hbm, z_hbm, wpb_hbm, wri_hbm, wro_hbm, wci_hbm, wco_hbm, wti_hbm, wto_hbm, out_hbm,
                 e_v, m_v, z_v, wpb_v, wri_v, wro_v, wci_v, wco_v, wti_v, wto_v,
                 bias32, bias_all, q_s, k_s, v_s, g_s, mb_s, hm_s, bias_t, gt_s, e1_send, e1_recv,
                 relay_v, wc_s, mrow_s, qsum_s, kt_s, vt_s, gc_s, x_s, p3_s, co_s, out_v,
                 in_sem, out_sem, chain_sem, pair_sem, bias_sem, send_sem, recv_sem, relay_sem, hand_sem):
    n_dev, n_seq, n_res, ch, heads = dims
    chips = n_dev // 2
    reach = chips // 2
    blk = n_res // n_dev
    hd = ch // heads
    c2 = hd ** -0.5 * LOG2E
    hrows = heads * blk
    half = blk // 2
    prows = n_seq * half
    me = lax.axis_index("seq")
    z, c = lax.div(me, 2), lax.rem(me, 2)

    def chip_at(offset):
        return lax.rem(z + offset + chips, chips)

    def slot_of(chip, core):
        return chip * 2 + core

    loads = [(z_hbm, z_v), (wpb_hbm, wpb_v), (e_hbm, e_v), (m_hbm, m_v), (wri_hbm, wri_v), (wro_hbm, wro_v),
             (wci_hbm, wci_v), (wco_hbm, wco_v), (wti_hbm, wti_v), (wto_hbm, wto_v)]
    copies = [pltpu.make_async_copy(src, dst, in_sem.at[n]) for n, (src, dst) in enumerate(loads)]
    for copy in copies:
        copy.start()

    barrier = pltpu.get_barrier_semaphore()
    for d in range(1, n_dev):
        pl.semaphore_signal(barrier, inc=1, device_id={"seq": lax.rem(me + d, n_dev)}, device_id_type=MESH)

    copies[0].wait()
    copies[1].wait()
    wpb_t = wpb_v[...]

    def bias_row(i, carry):
        rows = dot_nt(wpb_t, layer_norm(z_v[i]))
        for n in range(n_res // 128):
            bias32[n, pl.ds(i, heads, stride=blk), :] = rows[:, n * 128:(n + 1) * 128]
        return carry

    lax.fori_loop(0, blk, bias_row, 0, unroll=True)
    bias_all[me, :hrows] = jnp.concatenate([bias32[n] for n in range(n_res // 128)], axis=-1).astype(BF16)
    copies[3].wait()
    m_f32 = m_v[...].astype(F32)
    mb_s[...] = (MASK_BIG * LOG2E) * (m_f32 - 1.0)
    bias_all[me, hrows:] = jnp.concatenate([m_f32, m_f32], axis=0).astype(BF16)
    pl.semaphore_wait(barrier, n_dev - 1)

    def bias_copy(slot, sem, chip, core):
        return pltpu.make_async_remote_copy(
            src_ref=bias_all.at[slot], dst_ref=bias_all.at[slot], send_sem=sem, recv_sem=bias_sem.at[slot],
            device_id={"seq": slot_of(chip, core)}, device_id_type=MESH)

    def up(k):
        return bias_copy(slot_of(chip_at(-k), c), chain_sem.at[0, k], chip_at(1), c)

    def down(k):
        return bias_copy(slot_of(chip_at(k), c), chain_sem.at[1, k], chip_at(-1), c)

    def across(offset, t):
        return bias_copy(slot_of(chip_at(offset), c), pair_sem.at[t], z, 1 - c)

    def bias_wait(offset, core):
        bias_copy(slot_of(chip_at(offset), core), pair_sem.at[0], z, c).wait_recv()

    up(0).start()
    down(0).start()
    across(0, 0).start()

    for h in range(heads):
        hm_s[h] = jnp.where(lax.div(iota((blk, ch), 1), hd) == h, 1.0, 0.0).astype(BF16)
    copies[2].wait()
    copies[4].wait()

    def project(s, carry):
        proj = dot(layer_norm(e_v[s]), wri_v[...]).astype(BF16)
        q_s[s] = proj[:, :ch]
        k_s[s] = proj[:, ch:2 * ch]
        v_s[s] = proj[:, 2 * ch:3 * ch]
        g_s[s] = proj[:, 3 * ch:]
        return carry

    lax.fori_loop(0, n_seq, project, 0, unroll=True)
    copies[5].wait()

    lane_head = lax.div(iota((blk, ch), 1), hd)

    def own_head(blocks):
        picked = blocks[0]
        for h in range(1, heads):
            picked = jnp.where(lane_head == h, blocks[h], picked)
        return picked

    def e1_copy(t, core, hf):
        return pltpu.make_async_remote_copy(
            src_ref=e1_send.at[t, hf, core], dst_ref=e1_recv.at[hf, me], send_sem=send_sem.at[t, hf, core],
            recv_sem=recv_sem.at[hf, me], device_id={"seq": slot_of(tile_chip(t), core)}, device_id_type=MESH)

    def hand_over(core, hf):
        return pltpu.make_async_remote_copy(
            src_ref=e1_send.at[chips - 1, hf, core], dst_ref=relay_v.at[core, hf], send_sem=send_sem.at[chips - 1, hf, core],
            recv_sem=relay_sem.at[core, hf], device_id={"seq": slot_of(chip_at(1 - 2 * core), c)}, device_id_type=MESH)

    def hand_on(core, hf):
        way = 1 - 2 * core
        source = slot_of(chip_at(-way), c)
        return pltpu.make_async_remote_copy(
            src_ref=relay_v.at[core, hf], dst_ref=e1_recv.at[hf, source], send_sem=hand_sem.at[core, hf],
            recv_sem=recv_sem.at[hf, source], device_id={"seq": slot_of(chip_at(way * (reach - 1)), core)}, device_id_type=MESH)

    def relay(hf):
        for core in range(2):
            hand_over(core, hf).wait_recv()
            hand_on(core, hf).start()

    def tile_offset(t):
        k = lax.div(t + 1, 2)
        return k * (1 - 2 * lax.rem(t, 2))

    def tile_chip(t):
        return chip_at(tile_offset(t))

    def row_tile(t, carry):
        k = lax.div(t + 1, 2)

        @pl.when(lax.rem(t, 2) == 1)
        def _():
            bias_wait(-k, c)
            across(-k, t).start()

            @pl.when(k < reach)
            def _():
                up(k).start()
                bias_wait(k, c)
                across(k, t + 1).start()

            @pl.when(k < reach - 1)
            def _():
                down(k).start()

        bias_wait(tile_offset(t), 1 - c)
        chip = tile_chip(t)
        for core in range(2):
            bias_t[core * hrows:(core + 1) * hrows] = bias_all[slot_of(chip, core), :hrows].astype(F32) * LOG2E
        first = pl.multiple_of(chip * (2 * blk), 2 * blk)

        def logits_of(s):
            parts = []
            for core in range(2):
                q_rows = q_s[s, pl.ds(first + core * blk, blk), :]
                parts += [q_rows * hm_s[h] for h in range(heads)]
            return dot_nt(jnp.concatenate(parts, axis=0), k_s[s])

        logits = logits_of(0)
        for s in range(n_seq):
            ahead = logits_of(s + 1) if s + 1 < n_seq else None
            mask_row = mb_s[s:s + 1, :]
            probs = []
            step = hrows // 2
            for r in range(0, 2 * hrows, step):
                x = logits[r:r + step] * c2 + (bias_t[r:r + step] + mask_row)
                p = jnp.exp2(x - jnp.max(x, axis=-1, keepdims=True))
                probs.append((p * (1.0 / jnp.sum(p, axis=-1, keepdims=True))).astype(BF16))
            attended = dot(jnp.concatenate(probs, axis=0), v_s[s])
            for core in range(2):
                o = own_head([attended[core * hrows + h * blk:core * hrows + (h + 1) * blk] for h in range(heads)])
                gate = jax.nn.sigmoid(g_s[s, pl.ds(first + core * blk, blk), :].astype(F32))
                gated = gate * o
                for hf in range(2):
                    gt_s[hf, core, s] = gated[hf * half:(hf + 1) * half]
            logits = ahead
        update = dot(gt_s[...].reshape(4 * prows, ch).astype(BF16), wro_v[...])
        for core in range(2):
            e_rows = e_v[:, pl.ds(first + core * blk, blk), :].astype(F32)
            for hf in range(2):
                r = (hf * 2 + core) * prows
                e_half = e_rows[:, hf * half:(hf + 1) * half, :].reshape(prows, ch)
                e1_send[t, hf, core] = (e_half + update[r:r + prows]).astype(BF16)

        @pl.when(t == 0)
        def _():
            for hf in range(2):
                e1_recv[hf, me] = e1_send[0, hf, c]
                e1_copy(0, 1 - c, hf).start()

        @pl.when(jnp.logical_and(t > 0, t < chips - 1))
        def _():
            e1_copy(t, 0, 0).start()
            e1_copy(t, 1, 0).start()

        return carry

    lax.fori_loop(0, chips, row_tile, 0)
    for hf in range(2):
        for core in range(2):
            hand_over(core, hf).start()

    def second_halves(first_t, last_t):
        for t in range(first_t, last_t):
            for core in range(2):
                e1_copy(t, core, 1).start()

    second_halves(1, 3)

    copies[6].wait()
    w_k, w_v = wci_v[ch:ch + hd], wci_v[ch + hd:ch + 2 * hd]
    w_all = jnp.concatenate([wci_v[:ch]] + [w_k] * heads + [w_v] * heads + [wci_v[ch + 2 * hd:]], axis=0)
    eye = jnp.where(iota((ch, ch), 0) == iota((ch, ch), 1), 1.0, 0.0).astype(BF16)
    wc_s[...] = dot_nt(eye, w_all).astype(BF16)

    pad = 2 * n_seq
    m_all = bias_all[:, hrows:, :].reshape(n_dev * pad, n_res)
    lane = iota((n_res, 2 * prows), 1)
    row = iota((n_dev * pad, 2 * prows), 0)
    col = iota((n_dev * pad, 2 * prows), 1)
    own = jnp.logical_and(lax.rem(row, pad) == lax.div(lax.rem(col, prows), half), lax.rem(lax.div(row, pad), 2) == lax.div(col, prows))
    for hf in range(2):
        pick = jnp.where(iota((n_res, 2 * prows), 0) == me * blk + hf * half + lax.rem(lane, half), 1.0, 0.0).astype(BF16)
        m_sel = jnp.where(own, dot(m_all, pick), 0.0)
        mrow_s[hf] = jnp.sum(m_sel.reshape(chips, 2 * pad, 2 * prows), axis=1)
    qsum_s[...] = jnp.zeros_like(qsum_s)
    width = 4 * prows
    same = lax.rem(iota((half, width), 1), half) == iota((half, width), 0)
    same_h = lax.rem(iota((heads * half, width), 1), half) == lax.rem(iota((heads * half, width), 0), half)

    def lane_mask(hf, chip_a, chip_b):
        return jnp.concatenate([mrow_s[hf, pl.ds(chip, 1), :] for chip in (chip_a, chip_b)], axis=1)

    def column_in(hf, j):
        sources = [chip_at(-tile_offset(t)) for t in (2 * j, 2 * j + 1)]

        def arrival(chip, core):
            slot = slot_of(chip, core)
            pltpu.make_async_remote_copy(
                src_ref=e1_send.at[0, 0, 0], dst_ref=e1_recv.at[hf, slot], send_sem=send_sem.at[0, 0, 0],
                recv_sem=recv_sem.at[hf, slot], device_id={"seq": me}, device_id_type=MESH).wait_recv()

        if j == 0:
            arrival(sources[0], 1 - c)
        else:
            arrival(sources[0], 0)
            arrival(sources[0], 1)
        arrival(sources[1], 0)
        arrival(sources[1], 1)
        rows = jnp.concatenate([e1_recv[hf, pl.ds(chip * 2, 2)].reshape(2 * prows, ch) for chip in sources], axis=0)
        proj = dot(layer_norm(rows), wc_s[...]).astype(BF16)
        for n, chip in enumerate(sources):
            part = proj[n * 2 * prows:(n + 1) * 2 * prows]
            kt_s[hf, chip] = part[:, ch:2 * ch]
            vt_s[hf, chip] = part[:, 2 * ch:3 * ch]
            gc_s[hf, chip] = part[:, 3 * ch:]
        sel = jnp.where(same, lane_mask(hf, sources[0], sources[1]), 0.0).astype(BF16)
        qsum_s[hf] += dot(sel, proj[:, :ch])

    def column_attention(hf):
        count = jnp.sum(mrow_s[hf], axis=0, keepdims=True)
        count = jnp.sum(jnp.where(same[:, :2 * prows], count, 0.0), axis=-1, keepdims=True)
        q_mean = (qsum_s[hf] / (count + MEAN_EPS)).astype(BF16).astype(F32)
        q_rows = jnp.concatenate([q_mean * hm_s[h, :half].astype(F32) for h in range(heads)], axis=0).astype(BF16)
        n_rows = heads * half
        top = jnp.full((n_rows, width), EXCLUDED, F32)
        for pair in range(chips // 2):
            keys = kt_s[hf, 2 * pair:2 * pair + 2].reshape(width, ch)
            x = dot_nt(q_rows, keys) * c2 + (MASK_BIG * LOG2E) * (lane_mask(hf, 2 * pair, 2 * pair + 1) - 1.0)
            x = jnp.where(same_h, x, EXCLUDED)
            x_s[pair] = x
            top = jnp.maximum(top, x)
        top = jnp.max(top, axis=-1, keepdims=True)
        total = jnp.zeros((n_rows, width), F32)
        for pair in range(chips // 2):
            p = jnp.exp2(x_s[pair] - top)
            total = total + p
            for n in range(3):
                piece = p.astype(BF16)
                p3_s[n * n_rows:(n + 1) * n_rows, pair * width:(pair + 1) * width] = piece
                p = p - piece.astype(F32)
        o3 = dot(p3_s[...], vt_s[hf].reshape(chips * 2 * prows, ch))
        o = (o3[:n_rows] + o3[n_rows:2 * n_rows] + o3[2 * n_rows:]) / jnp.sum(total, axis=-1, keepdims=True)
        head = lane_head[:half]
        picked = o[:half]
        for h in range(1, heads):
            picked = jnp.where(head == h, o[h * half:(h + 1) * half], picked)
        co_s[...] = picked

    n_out = 4 * n_seq

    def out_copy(hf, pair):
        rows = pl.ds(pair * n_out, n_out)
        return pltpu.make_async_copy(out_v.at[hf, rows], out_hbm.at[rows, pl.ds(hf * half, half)], out_sem.at[hf, pair])

    def finish_pair(hf, pair):
        e1 = e1_recv[hf, pl.ds(pair * 4, 4)].reshape(width, ch).astype(F32)
        gate = jax.nn.sigmoid(gc_s[hf, pl.ds(pair * 2, 2)].reshape(width, ch).astype(F32)).reshape(n_out, half, ch)
        gated = (gate * co_s[...][None]).reshape(width, ch).astype(BF16)
        e2 = (e1 + dot(gated, wco_v[...])).astype(BF16)
        hidden = jnp.maximum(dot(layer_norm(e2), wti_v[...]), 0.0).astype(BF16)
        e3 = e2.astype(F32) + dot(hidden, wto_v[...])
        out_v[hf, pl.ds(pair * n_out, n_out)] = e3.reshape(n_out, half, ch).astype(BF16)
        out_copy(hf, pair).start()

    def finish(hf):
        def trip(n, carry):
            finish_pair(hf, 2 * n)
            finish_pair(hf, 2 * n + 1)
            return carry

        lax.fori_loop(0, chips // 4, trip, 0)

    relay(0)
    second_halves(3, 5)
    column_in(0, 0)
    column_in(0, 1)
    relay(1)
    second_halves(5, chips - 1)
    column_in(0, 2)
    column_in(0, 3)
    column_attention(0)
    copies[7].wait()
    copies[8].wait()
    copies[9].wait()
    finish(0)
    for j in range(chips // 2):
        column_in(1, j)
    column_attention(1)
    finish(1)

    for k in range(reach):
        up(k).wait_send()
        if k < reach - 1:
            down(k).wait_send()
    for t in range(chips):
        across(0, t).wait_send()
    for hf in range(2):
        e1_copy(0, 1 - c, hf).wait_send()
        for core in range(2):
            for t in range(1, chips - 1):
                e1_copy(t, core, hf).wait_send()
            hand_over(core, hf).wait_send()
            hand_on(core, hf).wait_send()
        for pair in range(chips // 2):
            out_copy(hf, pair).wait()


def solution(mesh):
    n_dev = mesh.shape["seq"]

    def local_block(e, m, z, w_pair_bias, w_row_in, w_row_out, w_col_in, w_col_out, w_trans_in, w_trans_out):
        n_seq, n_res, ch = e.shape
        heads = w_pair_bias.shape[1]
        blk = n_res // n_dev
        chips = n_dev // 2
        half = blk // 2
        hrows, prows = heads * blk, n_seq * half
        args = (e, m, z, w_pair_bias.T, w_row_in, w_row_out, w_col_in.T, w_col_out, w_trans_in, w_trans_out)
        scratch = [pltpu.VMEM(a.shape, a.dtype) for a in args] + [
            pltpu.VMEM((n_res // 128, hrows, 128), F32),
            pltpu.VMEM((n_dev, hrows + 2 * n_seq, n_res), BF16),
            pltpu.VMEM((n_seq, n_res, ch), BF16),
            pltpu.VMEM((n_seq, n_res, ch), BF16),
            pltpu.VMEM((n_seq, n_res, ch), BF16),
            pltpu.VMEM((n_seq, n_res, ch), BF16),
            pltpu.VMEM((n_seq, n_res), F32),
            pltpu.VMEM((heads, blk, ch), BF16),
            pltpu.VMEM((2 * hrows, n_res), F32),
            pltpu.VMEM((2, 2, n_seq, half, ch), F32),
            pltpu.VMEM((chips, 2, 2, prows, ch), BF16),
            pltpu.VMEM((2, n_dev, prows, ch), BF16),
            pltpu.VMEM((2, 2, prows, ch), BF16),
            pltpu.VMEM((ch, 4 * ch), BF16),
            pltpu.VMEM((2, chips, 2 * prows), F32),
            pltpu.VMEM((2, half, ch), F32),
            pltpu.VMEM((2, chips, 2 * prows, ch), BF16),
            pltpu.VMEM((2, chips, 2 * prows, ch), BF16),
            pltpu.VMEM((2, chips, 2 * prows, ch), BF16),
            pltpu.VMEM((chips // 2, heads * half, 4 * prows), F32),
            pltpu.VMEM((3 * heads * half, n_dev * prows), BF16),
            pltpu.VMEM((half, ch), F32),
            pltpu.VMEM((2, n_dev * n_seq, half, ch), BF16),
            pltpu.SemaphoreType.DMA((len(args),)),
            pltpu.SemaphoreType.DMA((2, chips // 2)),
            pltpu.SemaphoreType.DMA((2, chips // 2)),
            pltpu.SemaphoreType.DMA((chips,)),
            pltpu.SemaphoreType.DMA((n_dev,)),
            pltpu.SemaphoreType.DMA((chips, 2, 2)),
            pltpu.SemaphoreType.DMA((2, n_dev)),
            pltpu.SemaphoreType.DMA((2, 2)),
            pltpu.SemaphoreType.DMA((2, 2)),
        ]
        return pl.pallas_call(
            functools.partial(block_kernel, (n_dev, n_seq, n_res, ch, heads)),
            out_shape=jax.ShapeDtypeStruct((n_dev * n_seq, blk, ch), BF16),
            in_specs=[pl.BlockSpec(memory_space=pl.ANY)] * len(args),
            out_specs=pl.BlockSpec(memory_space=pl.ANY),
            scratch_shapes=scratch,
            name="msa_block",
            compiler_params=pltpu.CompilerParams(collective_id=0, has_side_effects=True, vmem_limit_bytes=60 * 2 ** 20),
        )(*args)

    rows_spec = P(('batch', 'seq'))
    return jax.shard_map(local_block, mesh=mesh, in_specs=(rows_spec, rows_spec, rows_spec, P(), P(), P(), P(), P(), P(), P()), out_specs=P('batch', 'seq'), check_vma=False)
```

```python
import functools

import jax
import jax.numpy as jnp
from jax import lax
from jax.experimental import pallas as pl
from jax.experimental.pallas import tpu as pltpu
from jax.sharding import PartitionSpec as P

MESH = pl.DeviceIdType.MESH
LN_EPS = 1.0e-5
MASK_BIG = 1.0e9
MEAN_EPS = 1.0e-10
LOG2E = 1.4426950408889634
EXCLUDED = -3.0e38
F32 = jnp.float32
BF16 = jnp.bfloat16
NT = (((1,), (1,)), ((), ()))


def layer_norm(x_in):
    x = x_in.astype(F32)
    centered = x - jnp.mean(x, axis=-1, keepdims=True)
    var = jnp.mean(centered * centered, axis=-1, keepdims=True)
    return (centered * lax.rsqrt(var + LN_EPS)).astype(BF16)


def dot(a, b):
    return jnp.dot(a, b, preferred_element_type=F32)


def dot_nt(a, b):
    return lax.dot_general(a, b, NT, preferred_element_type=F32)


def iota(shape, dim):
    return lax.broadcasted_iota(jnp.int32, shape, dim)


def block_kernel(dims, e_hbm, m_hbm, z_hbm, wpb_hbm, wri_hbm, wro_hbm, wci_hbm, wco_hbm, wti_hbm, wto_hbm, out_hbm,
                 e_v, m_v, z_v, wpb_v, wri_v, wro_v, wci_v, wco_v, wti_v, wto_v,
                 bias32, bias_all, q_s, k_s, v_s, g_s, mb_s, hm_s, bias_t, gt_s, e1_send, e1_recv,
                 wc_s, mrow_s, qsum_s, kt_s, vt_s, gc_s, x_s, p3_s, co_s, out_v,
                 in_sem, out_sem, chain_sem, pair_sem, bias_sem, send_sem, recv_sem):
    n_dev, n_seq, n_res, ch, heads = dims
    chips = n_dev // 2
    reach = chips // 2
    blk = n_res // n_dev
    hd = ch // heads
    c2 = hd ** -0.5 * LOG2E
    hrows = heads * blk
    half = blk // 2
    prows = n_seq * half
    me = lax.axis_index("seq")
    z, c = lax.div(me, 2), lax.rem(me, 2)

    def chip_at(offset):
        return lax.rem(z + offset + chips, chips)

    def slot_of(chip, core):
        return chip * 2 + core

    loads = [(z_hbm, z_v), (wpb_hbm, wpb_v), (e_hbm, e_v), (m_hbm, m_v), (wri_hbm, wri_v), (wro_hbm, wro_v),
             (wci_hbm, wci_v), (wco_hbm, wco_v), (wti_hbm, wti_v), (wto_hbm, wto_v)]
    copies = [pltpu.make_async_copy(src, dst, in_sem.at[n]) for n, (src, dst) in enumerate(loads)]
    for copy in copies:
        copy.start()

    barrier = pltpu.get_barrier_semaphore()
    for d in range(1, n_dev):
        pl.semaphore_signal(barrier, inc=1, device_id={"seq": lax.rem(me + d, n_dev)}, device_id_type=MESH)

    copies[0].wait()
    copies[1].wait()
    wpb_t = wpb_v[...]

    def bias_row(i, carry):
        rows = dot_nt(wpb_t, layer_norm(z_v[i]))
        for n in range(n_res // 128):
            bias32[n, pl.ds(i, heads, stride=blk), :] = rows[:, n * 128:(n + 1) * 128]
        return carry

    lax.fori_loop(0, blk, bias_row, 0, unroll=True)
    bias_all[me, :hrows] = jnp.concatenate([bias32[n] for n in range(n_res // 128)], axis=-1).astype(BF16)
    copies[3].wait()
    m_f32 = m_v[...].astype(F32)
    mb_s[...] = (MASK_BIG * LOG2E) * (m_f32 - 1.0)
    bias_all[me, hrows:] = jnp.concatenate([m_f32, m_f32], axis=0).astype(BF16)
    pl.semaphore_wait(barrier, n_dev - 1)

    def bias_copy(slot, sem, chip, core):
        return pltpu.make_async_remote_copy(
            src_ref=bias_all.at[slot], dst_ref=bias_all.at[slot], send_sem=sem, recv_sem=bias_sem.at[slot],
            device_id={"seq": slot_of(chip, core)}, device_id_type=MESH)

    def up(k):
        return bias_copy(slot_of(chip_at(-k), c), chain_sem.at[0, k], chip_at(1), c)

    def down(k):
        return bias_copy(slot_of(chip_at(k), c), chain_sem.at[1, k], chip_at(-1), c)

    def across(offset, t):
        return bias_copy(slot_of(chip_at(offset), c), pair_sem.at[t], z, 1 - c)

    def bias_wait(offset, core):
        bias_copy(slot_of(chip_at(offset), core), pair_sem.at[0], z, c).wait_recv()

    up(0).start()
    down(0).start()
    across(0, 0).start()

    for h in range(heads):
        hm_s[h] = jnp.where(lax.div(iota((blk, ch), 1), hd) == h, 1.0, 0.0).astype(BF16)
    copies[2].wait()
    copies[4].wait()

    def project(s, carry):
        proj = dot(layer_norm(e_v[s]), wri_v[...]).astype(BF16)
        q_s[s] = proj[:, :ch]
        k_s[s] = proj[:, ch:2 * ch]
        v_s[s] = proj[:, 2 * ch:3 * ch]
        g_s[s] = proj[:, 3 * ch:]
        return carry

    lax.fori_loop(0, n_seq, project, 0, unroll=True)
    copies[5].wait()

    lane_head = lax.div(iota((blk, ch), 1), hd)

    def own_head(blocks):
        picked = blocks[0]
        for h in range(1, heads):
            picked = jnp.where(lane_head == h, blocks[h], picked)
        return picked

    def e1_copy(t, core, hf):
        return pltpu.make_async_remote_copy(
            src_ref=e1_send.at[t, hf, core], dst_ref=e1_recv.at[hf, me], send_sem=send_sem.at[t, hf, core],
            recv_sem=recv_sem.at[hf, me], device_id={"seq": slot_of(tile_chip(t), core)}, device_id_type=MESH)

    def tile_offset(t):
        k = lax.div(t + 1, 2)
        return k * (2 * lax.rem(t, 2) - 1)

    def tile_chip(t):
        return chip_at(tile_offset(t))

    def row_tile(t, carry):
        k = lax.div(t, 2) + 1

        @pl.when(lax.rem(t, 2) == 0)
        def _():
            bias_wait(-k, c)

            @pl.when(k < reach)
            def _():
                up(k).start()

            across(-k, 2 * k - 1).start()

            @pl.when(k < reach)
            def _():
                bias_wait(k, c)

            @pl.when(k < reach - 1)
            def _():
                down(k).start()

            @pl.when(k < reach)
            def _():
                across(k, 2 * k).start()

        bias_wait(tile_offset(t), 1 - c)
        chip = tile_chip(t)
        for core in range(2):
            bias_t[core * hrows:(core + 1) * hrows] = bias_all[slot_of(chip, core), :hrows].astype(F32) * LOG2E
        first = pl.multiple_of(chip * (2 * blk), 2 * blk)

        def logits_of(s):
            parts = []
            for core in range(2):
                q_rows = q_s[s, pl.ds(first + core * blk, blk), :]
                parts += [q_rows * hm_s[h] for h in range(heads)]
            return dot_nt(jnp.concatenate(parts, axis=0), k_s[s])

        logits = logits_of(0)
        for s in range(n_seq):
            ahead = logits_of(s + 1) if s + 1 < n_seq else None
            mask_row = mb_s[s:s + 1, :]
            probs = []
            step = hrows // 2
            for r in range(0, 2 * hrows, step):
                x = logits[r:r + step] * c2 + (bias_t[r:r + step] + mask_row)
                p = jnp.exp2(x - jnp.max(x, axis=-1, keepdims=True))
                probs.append((p * (1.0 / jnp.sum(p, axis=-1, keepdims=True))).astype(BF16))
            attended = dot(jnp.concatenate(probs, axis=0), v_s[s])
            for core in range(2):
                o = own_head([attended[core * hrows + h * blk:core * hrows + (h + 1) * blk] for h in range(heads)])
                gate = jax.nn.sigmoid(g_s[s, pl.ds(first + core * blk, blk), :].astype(F32))
                gated = gate * o
                for hf in range(2):
                    gt_s[hf, core, s] = gated[hf * half:(hf + 1) * half]
            logits = ahead
        update = dot(gt_s[...].reshape(4 * prows, ch).astype(BF16), wro_v[...])
        for core in range(2):
            e_rows = e_v[:, pl.ds(first + core * blk, blk), :].astype(F32)
            for hf in range(2):
                r = (hf * 2 + core) * prows
                e_half = e_rows[:, hf * half:(hf + 1) * half, :].reshape(prows, ch)
                e1_send[t, hf, core] = (e_half + update[r:r + prows]).astype(BF16)

        @pl.when(t == 0)
        def _():
            for hf in range(2):
                e1_recv[hf, me] = e1_send[0, hf, c]
                e1_copy(0, 1 - c, hf).start()

        @pl.when(t > 0)
        def _():
            e1_copy(t, 0, 0).start()
            e1_copy(t, 1, 0).start()

        @pl.when(jnp.logical_and(t > 0, t < 5))
        def _():
            e1_copy(t, 0, 1).start()
            e1_copy(t, 1, 1).start()

        return carry

    lax.fori_loop(0, chips, row_tile, 0)
    def second_halves(first_t, last_t):
        for t in range(first_t, last_t):
            for core in range(2):
                e1_copy(t, core, 1).start()

    second_halves(5, chips)

    copies[6].wait()
    w_k, w_v = wci_v[ch:ch + hd], wci_v[ch + hd:ch + 2 * hd]
    w_all = jnp.concatenate([wci_v[:ch]] + [w_k] * heads + [w_v] * heads + [wci_v[ch + 2 * hd:]], axis=0)
    eye = jnp.where(iota((ch, ch), 0) == iota((ch, ch), 1), 1.0, 0.0).astype(BF16)
    wc_s[...] = dot_nt(eye, w_all).astype(BF16)

    pad = 2 * n_seq
    m_all = bias_all[:, hrows:, :].reshape(n_dev * pad, n_res)
    lane = iota((n_res, 2 * prows), 1)
    row = iota((n_dev * pad, 2 * prows), 0)
    col = iota((n_dev * pad, 2 * prows), 1)
    own = jnp.logical_and(lax.rem(row, pad) == lax.div(lax.rem(col, prows), half), lax.rem(lax.div(row, pad), 2) == lax.div(col, prows))
    for hf in range(2):
        pick = jnp.where(iota((n_res, 2 * prows), 0) == me * blk + hf * half + lax.rem(lane, half), 1.0, 0.0).astype(BF16)
        m_sel = jnp.where(own, dot(m_all, pick), 0.0)
        mrow_s[hf] = jnp.sum(m_sel.reshape(chips, 2 * pad, 2 * prows), axis=1)
    qsum_s[...] = jnp.zeros_like(qsum_s)
    width = 4 * prows
    same = lax.rem(iota((half, width), 1), half) == iota((half, width), 0)
    same_h = lax.rem(iota((heads * half, width), 1), half) == lax.rem(iota((heads * half, width), 0), half)

    def lane_mask(hf, chip_a, chip_b):
        return jnp.concatenate([mrow_s[hf, pl.ds(chip, 1), :] for chip in (chip_a, chip_b)], axis=1)

    def column_in(hf, j):
        sources = [chip_at(-tile_offset(t)) for t in (2 * j, 2 * j + 1)]

        def arrival(chip, core):
            slot = slot_of(chip, core)
            pltpu.make_async_remote_copy(
                src_ref=e1_send.at[0, 0, 0], dst_ref=e1_recv.at[hf, slot], send_sem=send_sem.at[0, 0, 0],
                recv_sem=recv_sem.at[hf, slot], device_id={"seq": me}, device_id_type=MESH).wait_recv()

        if j == 0:
            arrival(sources[0], 1 - c)
        else:
            arrival(sources[0], 0)
            arrival(sources[0], 1)
        arrival(sources[1], 0)
        arrival(sources[1], 1)
        rows = jnp.concatenate([e1_recv[hf, pl.ds(chip * 2, 2)].reshape(2 * prows, ch) for chip in sources], axis=0)
        proj = dot(layer_norm(rows), wc_s[...]).astype(BF16)
        for n, chip in enumerate(sources):
            part = proj[n * 2 * prows:(n + 1) * 2 * prows]
            kt_s[hf, chip] = part[:, ch:2 * ch]
            vt_s[hf, chip] = part[:, 2 * ch:3 * ch]
            gc_s[hf, chip] = part[:, 3 * ch:]
        sel = jnp.where(same, lane_mask(hf, sources[0], sources[1]), 0.0).astype(BF16)
        qsum_s[hf] += dot(sel, proj[:, :ch])

    def column_attention(hf):
        count = jnp.sum(mrow_s[hf], axis=0, keepdims=True)
        count = jnp.sum(jnp.where(same[:, :2 * prows], count, 0.0), axis=-1, keepdims=True)
        q_mean = (qsum_s[hf] / (count + MEAN_EPS)).astype(BF16).astype(F32)
        q_rows = jnp.concatenate([q_mean * hm_s[h, :half].astype(F32) for h in range(heads)], axis=0).astype(BF16)
        n_rows = heads * half
        top = jnp.full((n_rows, width), EXCLUDED, F32)
        for pair in range(chips // 2):
            keys = kt_s[hf, 2 * pair:2 * pair + 2].reshape(width, ch)
            x = dot_nt(q_rows, keys) * c2 + (MASK_BIG * LOG2E) * (lane_mask(hf, 2 * pair, 2 * pair + 1) - 1.0)
            x = jnp.where(same_h, x, EXCLUDED)
            x_s[pair] = x
            top = jnp.maximum(top, x)
        top = jnp.max(top, axis=-1, keepdims=True)
        total = jnp.zeros((n_rows, width), F32)
        for pair in range(chips // 2):
            p = jnp.exp2(x_s[pair] - top)
            total = total + p
            for n in range(3):
                piece = p.astype(BF16)
                p3_s[n * n_rows:(n + 1) * n_rows, pair * width:(pair + 1) * width] = piece
                p = p - piece.astype(F32)
        o3 = dot(p3_s[...], vt_s[hf].reshape(chips * 2 * prows, ch))
        o = (o3[:n_rows] + o3[n_rows:2 * n_rows] + o3[2 * n_rows:]) / jnp.sum(total, axis=-1, keepdims=True)
        head = lane_head[:half]
        picked = o[:half]
        for h in range(1, heads):
            picked = jnp.where(head == h, o[h * half:(h + 1) * half], picked)
        co_s[...] = picked

    n_out = 4 * n_seq

    def out_copy(hf, pair):
        rows = pl.ds(pair * n_out, n_out)
        return pltpu.make_async_copy(out_v.at[hf, rows], out_hbm.at[rows, pl.ds(hf * half, half)], out_sem.at[hf, pair])

    def finish_pair(hf, pair):
        e1 = e1_recv[hf, pl.ds(pair * 4, 4)].reshape(width, ch).astype(F32)
        gate = jax.nn.sigmoid(gc_s[hf, pl.ds(pair * 2, 2)].reshape(width, ch).astype(F32)).reshape(n_out, half, ch)
        gated = (gate * co_s[...][None]).reshape(width, ch).astype(BF16)
        e2 = (e1 + dot(gated, wco_v[...])).astype(BF16)
        hidden = jnp.maximum(dot(layer_norm(e2), wti_v[...]), 0.0).astype(BF16)
        e3 = e2.astype(F32) + dot(hidden, wto_v[...])
        out_v[hf, pl.ds(pair * n_out, n_out)] = e3.reshape(n_out, half, ch).astype(BF16)
        out_copy(hf, pair).start()

    def finish(hf):
        def trip(n, carry):
            finish_pair(hf, 2 * n)
            finish_pair(hf, 2 * n + 1)
            return carry

        lax.fori_loop(0, chips // 4, trip, 0)

    column_in(0, 0)
    column_in(0, 1)
    column_in(0, 2)
    column_in(0, 3)
    column_attention(0)
    copies[7].wait()
    copies[8].wait()
    copies[9].wait()
    finish(0)
    for j in range(chips // 2):
        column_in(1, j)
    column_attention(1)
    finish(1)

    for k in range(reach):
        up(k).wait_send()
        if k < reach - 1:
            down(k).wait_send()
    for t in range(chips):
        across(0, t).wait_send()
    for hf in range(2):
        e1_copy(0, 1 - c, hf).wait_send()
        for core in range(2):
            for t in range(1, chips):
                e1_copy(t, core, hf).wait_send()
        for pair in range(chips // 2):
            out_copy(hf, pair).wait()


def solution(mesh):
    n_dev = mesh.shape["seq"]

    def local_block(e, m, z, w_pair_bias, w_row_in, w_row_out, w_col_in, w_col_out, w_trans_in, w_trans_out):
        n_seq, n_res, ch = e.shape
        heads = w_pair_bias.shape[1]
        blk = n_res // n_dev
        chips = n_dev // 2
        half = blk // 2
        hrows, prows = heads * blk, n_seq * half
        args = (e, m, z, w_pair_bias.T, w_row_in, w_row_out, w_col_in.T, w_col_out, w_trans_in, w_trans_out)
        scratch = [pltpu.VMEM(a.shape, a.dtype) for a in args] + [
            pltpu.VMEM((n_res // 128, hrows, 128), F32),
            pltpu.VMEM((n_dev, hrows + 2 * n_seq, n_res), BF16),
            pltpu.VMEM((n_seq, n_res, ch), BF16),
            pltpu.VMEM((n_seq, n_res, ch), BF16),
            pltpu.VMEM((n_seq, n_res, ch), BF16),
            pltpu.VMEM((n_seq, n_res, ch), BF16),
            pltpu.VMEM((n_seq, n_res), F32),
            pltpu.VMEM((heads, blk, ch), BF16),
            pltpu.VMEM((2 * hrows, n_res), F32),
            pltpu.VMEM((2, 2, n_seq, half, ch), F32),
            pltpu.VMEM((chips, 2, 2, prows, ch), BF16),
            pltpu.VMEM((2, n_dev, prows, ch), BF16),
            pltpu.VMEM((ch, 4 * ch), BF16),
            pltpu.VMEM((2, chips, 2 * prows), F32),
            pltpu.VMEM((2, half, ch), F32),
            pltpu.VMEM((2, chips, 2 * prows, ch), BF16),
            pltpu.VMEM((2, chips, 2 * prows, ch), BF16),
            pltpu.VMEM((2, chips, 2 * prows, ch), BF16),
            pltpu.VMEM((chips // 2, heads * half, 4 * prows), F32),
            pltpu.VMEM((3 * heads * half, n_dev * prows), BF16),
            pltpu.VMEM((half, ch), F32),
            pltpu.VMEM((2, n_dev * n_seq, half, ch), BF16),
            pltpu.SemaphoreType.DMA((len(args),)),
            pltpu.SemaphoreType.DMA((2, chips // 2)),
            pltpu.SemaphoreType.DMA((2, chips // 2)),
            pltpu.SemaphoreType.DMA((chips,)),
            pltpu.SemaphoreType.DMA((n_dev,)),
            pltpu.SemaphoreType.DMA((chips, 2, 2)),
            pltpu.SemaphoreType.DMA((2, n_dev)),
        ]
        return pl.pallas_call(
            functools.partial(block_kernel, (n_dev, n_seq, n_res, ch, heads)),
            out_shape=jax.ShapeDtypeStruct((n_dev * n_seq, blk, ch), BF16),
            in_specs=[pl.BlockSpec(memory_space=pl.ANY)] * len(args),
            out_specs=pl.BlockSpec(memory_space=pl.ANY),
            scratch_shapes=scratch,
            name="msa_block",
            compiler_params=pltpu.CompilerParams(collective_id=0, has_side_effects=True, vmem_limit_bytes=60 * 2 ** 20),
        )(*args)

    rows_spec = P(('batch', 'seq'))
    return jax.shard_map(local_block, mesh=mesh, in_specs=(rows_spec, rows_spec, rows_spec, P(), P(), P(), P(), P(), P(), P()), out_specs=P('batch', 'seq'), check_vma=False)
```

```python
import functools

import jax
import jax.numpy as jnp
from jax import lax
from jax.experimental import pallas as pl
from jax.experimental.pallas import tpu as pltpu
from jax.sharding import PartitionSpec as P

MESH = pl.DeviceIdType.MESH
LN_EPS = 1.0e-5
MASK_BIG = 1.0e9
MEAN_EPS = 1.0e-10
LOG2E = 1.4426950408889634
EXCLUDED = -3.0e38
F32 = jnp.float32
BF16 = jnp.bfloat16
NT = (((1,), (1,)), ((), ()))


def layer_norm(x_in):
    x = x_in.astype(F32)
    centered = x - jnp.mean(x, axis=-1, keepdims=True)
    var = jnp.mean(centered * centered, axis=-1, keepdims=True)
    return (centered * lax.rsqrt(var + LN_EPS)).astype(BF16)


def dot(a, b):
    return jnp.dot(a, b, preferred_element_type=F32)


def dot_nt(a, b):
    return lax.dot_general(a, b, NT, preferred_element_type=F32)


def iota(shape, dim):
    return lax.broadcasted_iota(jnp.int32, shape, dim)


def block_kernel(dims, e_hbm, m_hbm, z_hbm, wpb_hbm, wri_hbm, wro_hbm, wci_hbm, wco_hbm, wti_hbm, wto_hbm, out_hbm,
                 e_v, m_v, z_v, wpb_v, wri_v, wro_v, wci_v, wco_v, wti_v, wto_v,
                 bias32, bias_all, q_s, k_s, v_s, g_s, mb_s, hm_s, bias_t, gt_s, e1_send, e1_recv,
                 wc_s, mrow_s, qsum_s, kt_s, vt_s, gc_s, x_s, p3_s, co_s, out_v,
                 in_sem, out_sem, chain_sem, pair_sem, bias_sem, send_sem, recv_sem):
    n_dev, n_seq, n_res, ch, heads = dims
    chips = n_dev // 2
    reach = chips // 2
    blk = n_res // n_dev
    hd = ch // heads
    c2 = hd ** -0.5 * LOG2E
    hrows = heads * blk
    half = blk // 2
    prows = n_seq * half
    me = lax.axis_index("seq")
    z, c = lax.div(me, 2), lax.rem(me, 2)

    def chip_at(offset):
        return lax.rem(z + offset + chips, chips)

    def slot_of(chip, core):
        return chip * 2 + core

    loads = [(z_hbm, z_v), (wpb_hbm, wpb_v), (e_hbm, e_v), (m_hbm, m_v), (wri_hbm, wri_v), (wro_hbm, wro_v),
             (wci_hbm, wci_v), (wco_hbm, wco_v), (wti_hbm, wti_v), (wto_hbm, wto_v)]
    copies = [pltpu.make_async_copy(src, dst, in_sem.at[n]) for n, (src, dst) in enumerate(loads)]
    for copy in copies:
        copy.start()

    barrier = pltpu.get_barrier_semaphore()
    for d in range(1, n_dev):
        pl.semaphore_signal(barrier, inc=1, device_id={"seq": lax.rem(me + d, n_dev)}, device_id_type=MESH)

    copies[0].wait()
    copies[1].wait()
    wpb_t = wpb_v[...]
    ones = jnp.ones((z_v.shape[2], z_v.shape[2]), BF16)

    def bias_row(i, carry):
        z_row = z_v[i]
        centered = z_row.astype(F32) - dot(z_row, ones) * (1.0 / z_row.shape[1])
        var = jnp.mean(centered * centered, axis=-1, keepdims=True)
        rows = dot_nt(wpb_t, (centered * lax.rsqrt(var + LN_EPS)).astype(BF16))
        for n in range(n_res // 128):
            bias32[n, pl.ds(i, heads, stride=blk), :] = rows[:, n * 128:(n + 1) * 128]
        return carry

    lax.fori_loop(0, blk, bias_row, 0, unroll=True)
    bias_all[me, :hrows] = jnp.concatenate([bias32[n] for n in range(n_res // 128)], axis=-1).astype(BF16)
    copies[3].wait()
    m_f32 = m_v[...].astype(F32)
    mb_s[...] = (MASK_BIG * LOG2E) * (m_f32 - 1.0)
    bias_all[me, hrows:] = jnp.concatenate([m_f32, m_f32], axis=0).astype(BF16)
    pl.semaphore_wait(barrier, n_dev - 1)

    def bias_copy(slot, sem, chip, core):
        return pltpu.make_async_remote_copy(
            src_ref=bias_all.at[slot], dst_ref=bias_all.at[slot], send_sem=sem, recv_sem=bias_sem.at[slot],
            device_id={"seq": slot_of(chip, core)}, device_id_type=MESH)

    def up(k):
        return bias_copy(slot_of(chip_at(-k), c), chain_sem.at[0, k], chip_at(1), c)

    def down(k):
        return bias_copy(slot_of(chip_at(k), c), chain_sem.at[1, k], chip_at(-1), c)

    def across(offset, t):
        return bias_copy(slot_of(chip_at(offset), c), pair_sem.at[t], z, 1 - c)

    def bias_wait(offset, core):
        bias_copy(slot_of(chip_at(offset), core), pair_sem.at[0], z, c).wait_recv()

    up(0).start()
    down(0).start()
    across(0, 0).start()

    for h in range(heads):
        hm_s[h] = jnp.where(lax.div(iota((blk, ch), 1), hd) == h, 1.0, 0.0).astype(BF16)
    copies[2].wait()
    copies[4].wait()

    def project(s, carry):
        proj = dot(layer_norm(e_v[s]), wri_v[...]).astype(BF16)
        q_s[s] = proj[:, :ch]
        k_s[s] = proj[:, ch:2 * ch]
        v_s[s] = proj[:, 2 * ch:3 * ch]
        g_s[s] = proj[:, 3 * ch:]
        return carry

    lax.fori_loop(0, n_seq, project, 0, unroll=True)
    copies[5].wait()

    lane_head = lax.div(iota((blk, ch), 1), hd)

    def own_head(blocks):
        picked = blocks[0]
        for h in range(1, heads):
            picked = jnp.where(lane_head == h, blocks[h], picked)
        return picked

    def e1_copy(t, core, hf):
        return pltpu.make_async_remote_copy(
            src_ref=e1_send.at[t, hf, core], dst_ref=e1_recv.at[hf, me], send_sem=send_sem.at[t, hf, core],
            recv_sem=recv_sem.at[hf, me], device_id={"seq": slot_of(tile_chip(t), core)}, device_id_type=MESH)

    def tile_offset(t):
        k = lax.div(t + 1, 2)
        return k * (2 * lax.rem(t, 2) - 1)

    def tile_chip(t):
        return chip_at(tile_offset(t))

    def send(t, hf):
        for core in range(2):
            e1_copy(t, core, hf).start()

    def row_tile(t, carry):
        k = lax.div(t, 2) + 1

        @pl.when(lax.rem(t, 2) == 0)
        def _():
            bias_wait(-k, c)

            @pl.when(k < reach)
            def _():
                up(k).start()

            across(-k, 2 * k - 1).start()

            @pl.when(k < reach)
            def _():
                bias_wait(k, c)

            @pl.when(k < reach - 1)
            def _():
                down(k).start()

            @pl.when(k < reach)
            def _():
                across(k, 2 * k).start()

            @pl.when(t == 2)
            def _():
                send(1, 0)

            @pl.when(t == 4)
            def _():
                send(3, 0)
                send(1, 1)
                send(2, 1)

        bias_wait(tile_offset(t), 1 - c)
        chip = tile_chip(t)
        for core in range(2):
            bias_t[core * hrows:(core + 1) * hrows] = bias_all[slot_of(chip, core), :hrows].astype(F32) * LOG2E
        first = pl.multiple_of(chip * (2 * blk), 2 * blk)

        def logits_of(s):
            parts = []
            for core in range(2):
                q_rows = q_s[s, pl.ds(first + core * blk, blk), :]
                parts += [q_rows * hm_s[h] for h in range(heads)]
            return dot_nt(jnp.concatenate(parts, axis=0), k_s[s])

        logits = logits_of(0)
        for s in range(n_seq):
            ahead = logits_of(s + 1) if s + 1 < n_seq else None
            mask_row = mb_s[s:s + 1, :]
            probs = []
            step = hrows // 2
            for r in range(0, 2 * hrows, step):
                x = logits[r:r + step] * c2 + (bias_t[r:r + step] + mask_row)
                p = jnp.exp2(x - jnp.max(x, axis=-1, keepdims=True))
                probs.append((p * (1.0 / jnp.sum(p, axis=-1, keepdims=True))).astype(BF16))
            attended = dot(jnp.concatenate(probs, axis=0), v_s[s])
            for core in range(2):
                o = own_head([attended[core * hrows + h * blk:core * hrows + (h + 1) * blk] for h in range(heads)])
                gate = jax.nn.sigmoid(g_s[s, pl.ds(first + core * blk, blk), :].astype(F32))
                gated = gate * o
                for hf in range(2):
                    gt_s[hf, core, s] = gated[hf * half:(hf + 1) * half]
            logits = ahead
        update = dot(gt_s[...].reshape(4 * prows, ch).astype(BF16), wro_v[...])
        for core in range(2):
            e_rows = e_v[:, pl.ds(first + core * blk, blk), :].astype(F32)
            for hf in range(2):
                r = (hf * 2 + core) * prows
                e_half = e_rows[:, hf * half:(hf + 1) * half, :].reshape(prows, ch)
                e1_send[t, hf, core] = (e_half + update[r:r + prows]).astype(BF16)

        @pl.when(t == 0)
        def _():
            for hf in range(2):
                e1_recv[hf, me] = e1_send[0, hf, c]
                e1_copy(0, 1 - c, hf).start()

        @pl.when(jnp.logical_or(t == 2, t > 3))
        def _():
            send(t, 0)

        return carry

    lax.fori_loop(0, chips, row_tile, 0)
    for t in range(3, chips):
        send(t, 1)

    copies[6].wait()
    w_k, w_v = wci_v[ch:ch + hd], wci_v[ch + hd:ch + 2 * hd]
    w_all = jnp.concatenate([wci_v[:ch]] + [w_k] * heads + [w_v] * heads + [wci_v[ch + 2 * hd:]], axis=0)
    eye = jnp.where(iota((ch, ch), 0) == iota((ch, ch), 1), 1.0, 0.0).astype(BF16)
    wc_s[...] = dot_nt(eye, w_all).astype(BF16)

    pad = 2 * n_seq
    m_all = bias_all[:, hrows:, :].reshape(n_dev * pad, n_res)
    lane = iota((n_res, 2 * prows), 1)
    row = iota((n_dev * pad, 2 * prows), 0)
    col = iota((n_dev * pad, 2 * prows), 1)
    own = jnp.logical_and(lax.rem(row, pad) == lax.div(lax.rem(col, prows), half), lax.rem(lax.div(row, pad), 2) == lax.div(col, prows))
    for hf in range(2):
        pick = jnp.where(iota((n_res, 2 * prows), 0) == me * blk + hf * half + lax.rem(lane, half), 1.0, 0.0).astype(BF16)
        m_sel = jnp.where(own, dot(m_all, pick), 0.0)
        mrow_s[hf] = jnp.sum(m_sel.reshape(chips, 2 * pad, 2 * prows), axis=1)
    qsum_s[...] = jnp.zeros_like(qsum_s)
    width = 4 * prows
    same = lax.rem(iota((half, width), 1), half) == iota((half, width), 0)
    same_h = lax.rem(iota((heads * half, width), 1), half) == lax.rem(iota((heads * half, width), 0), half)

    def lane_mask(hf, chip_a, chip_b):
        return jnp.concatenate([mrow_s[hf, pl.ds(chip, 1), :] for chip in (chip_a, chip_b)], axis=1)

    def column_in(hf, j):
        sources = [chip_at(-tile_offset(t)) for t in (2 * j, 2 * j + 1)]

        def arrival(chip, core):
            slot = slot_of(chip, core)
            pltpu.make_async_remote_copy(
                src_ref=e1_send.at[0, 0, 0], dst_ref=e1_recv.at[hf, slot], send_sem=send_sem.at[0, 0, 0],
                recv_sem=recv_sem.at[hf, slot], device_id={"seq": me}, device_id_type=MESH).wait_recv()

        if j == 0:
            arrival(sources[0], 1 - c)
        else:
            arrival(sources[0], 0)
            arrival(sources[0], 1)
        arrival(sources[1], 0)
        arrival(sources[1], 1)
        rows = jnp.concatenate([e1_recv[hf, pl.ds(chip * 2, 2)].reshape(2 * prows, ch) for chip in sources], axis=0)
        proj = dot(layer_norm(rows), wc_s[...]).astype(BF16)
        for n, chip in enumerate(sources):
            part = proj[n * 2 * prows:(n + 1) * 2 * prows]
            kt_s[hf, chip] = part[:, ch:2 * ch]
            vt_s[hf, chip] = part[:, 2 * ch:3 * ch]
            gc_s[hf, chip] = part[:, 3 * ch:]
        sel = jnp.where(same, lane_mask(hf, sources[0], sources[1]), 0.0).astype(BF16)
        qsum_s[hf] += dot(sel, proj[:, :ch])

    def column_attention(hf):
        count = jnp.sum(mrow_s[hf], axis=0, keepdims=True)
        count = jnp.sum(jnp.where(same[:, :2 * prows], count, 0.0), axis=-1, keepdims=True)
        q_mean = (qsum_s[hf] / (count + MEAN_EPS)).astype(BF16).astype(F32)
        q_rows = jnp.concatenate([q_mean * hm_s[h, :half].astype(F32) for h in range(heads)], axis=0).astype(BF16)
        n_rows = heads * half
        top = jnp.full((n_rows, width), EXCLUDED, F32)
        for pair in range(chips // 2):
            keys = kt_s[hf, 2 * pair:2 * pair + 2].reshape(width, ch)
            x = dot_nt(q_rows, keys) * c2 + (MASK_BIG * LOG2E) * (lane_mask(hf, 2 * pair, 2 * pair + 1) - 1.0)
            x = jnp.where(same_h, x, EXCLUDED)
            x_s[pair] = x
            top = jnp.maximum(top, x)
        top = jnp.max(top, axis=-1, keepdims=True)
        total = jnp.zeros((n_rows, width), F32)
        for pair in range(chips // 2):
            p = jnp.exp2(x_s[pair] - top)
            total = total + p
            for n in range(3):
                piece = p.astype(BF16)
                p3_s[n * n_rows:(n + 1) * n_rows, pair * width:(pair + 1) * width] = piece
                p = p - piece.astype(F32)
        o3 = dot(p3_s[...], vt_s[hf].reshape(chips * 2 * prows, ch))
        o = (o3[:n_rows] + o3[n_rows:2 * n_rows] + o3[2 * n_rows:]) / jnp.sum(total, axis=-1, keepdims=True)
        head = lane_head[:half]
        picked = o[:half]
        for h in range(1, heads):
            picked = jnp.where(head == h, o[h * half:(h + 1) * half], picked)
        co_s[...] = picked

    n_out = 4 * n_seq

    def out_copy(hf, pair):
        rows = pl.ds(pair * n_out, n_out)
        return pltpu.make_async_copy(out_v.at[hf, rows], out_hbm.at[rows, pl.ds(hf * half, half)], out_sem.at[hf, pair])

    def finish_pair(hf, pair):
        e1 = e1_recv[hf, pl.ds(pair * 4, 4)].reshape(width, ch).astype(F32)
        gate = jax.nn.sigmoid(gc_s[hf, pl.ds(pair * 2, 2)].reshape(width, ch).astype(F32)).reshape(n_out, half, ch)
        gated = (gate * co_s[...][None]).reshape(width, ch).astype(BF16)
        e2 = (e1 + dot(gated, wco_v[...])).astype(BF16)
        hidden = jnp.maximum(dot(layer_norm(e2), wti_v[...]), 0.0).astype(BF16)
        e3 = e2.astype(F32) + dot(hidden, wto_v[...])
        out_v[hf, pl.ds(pair * n_out, n_out)] = e3.reshape(n_out, half, ch).astype(BF16)
        out_copy(hf, pair).start()

    def finish(hf):
        def trip(n, carry):
            finish_pair(hf, 2 * n)
            finish_pair(hf, 2 * n + 1)
            return carry

        lax.fori_loop(0, chips // 4, trip, 0)

    column_in(0, 0)
    column_in(0, 1)
    column_in(0, 2)
    column_in(0, 3)
    column_attention(0)
    copies[7].wait()
    copies[8].wait()
    copies[9].wait()
    finish(0)
    for j in range(chips // 2):
        column_in(1, j)
    column_attention(1)
    finish(1)

    for k in range(reach):
        up(k).wait_send()
        if k < reach - 1:
            down(k).wait_send()
    for t in range(chips):
        across(0, t).wait_send()
    for hf in range(2):
        e1_copy(0, 1 - c, hf).wait_send()
        for core in range(2):
            for t in range(1, chips):
                e1_copy(t, core, hf).wait_send()
        for pair in range(chips // 2):
            out_copy(hf, pair).wait()


def solution(mesh):
    n_dev = mesh.shape["seq"]

    def local_block(e, m, z, w_pair_bias, w_row_in, w_row_out, w_col_in, w_col_out, w_trans_in, w_trans_out):
        n_seq, n_res, ch = e.shape
        heads = w_pair_bias.shape[1]
        blk = n_res // n_dev
        chips = n_dev // 2
        half = blk // 2
        hrows, prows = heads * blk, n_seq * half
        args = (e, m, z, w_pair_bias.T, w_row_in, w_row_out, w_col_in.T, w_col_out, w_trans_in, w_trans_out)
        scratch = [pltpu.VMEM(a.shape, a.dtype) for a in args] + [
            pltpu.VMEM((n_res // 128, hrows, 128), F32),
            pltpu.VMEM((n_dev, hrows + 2 * n_seq, n_res), BF16),
            pltpu.VMEM((n_seq, n_res, ch), BF16),
            pltpu.VMEM((n_seq, n_res, ch), BF16),
            pltpu.VMEM((n_seq, n_res, ch), BF16),
            pltpu.VMEM((n_seq, n_res, ch), BF16),
            pltpu.VMEM((n_seq, n_res), F32),
            pltpu.VMEM((heads, blk, ch), BF16),
            pltpu.VMEM((2 * hrows, n_res), F32),
            pltpu.VMEM((2, 2, n_seq, half, ch), F32),
            pltpu.VMEM((chips, 2, 2, prows, ch), BF16),
            pltpu.VMEM((2, n_dev, prows, ch), BF16),
            pltpu.VMEM((ch, 4 * ch), BF16),
            pltpu.VMEM((2, chips, 2 * prows), F32),
            pltpu.VMEM((2, half, ch), F32),
            pltpu.VMEM((2, chips, 2 * prows, ch), BF16),
            pltpu.VMEM((2, chips, 2 * prows, ch), BF16),
            pltpu.VMEM((2, chips, 2 * prows, ch), BF16),
            pltpu.VMEM((chips // 2, heads * half, 4 * prows), F32),
            pltpu.VMEM((3 * heads * half, n_dev * prows), BF16),
            pltpu.VMEM((half, ch), F32),
            pltpu.VMEM((2, n_dev * n_seq, half, ch), BF16),
            pltpu.SemaphoreType.DMA((len(args),)),
            pltpu.SemaphoreType.DMA((2, chips // 2)),
            pltpu.SemaphoreType.DMA((2, chips // 2)),
            pltpu.SemaphoreType.DMA((chips,)),
            pltpu.SemaphoreType.DMA((n_dev,)),
            pltpu.SemaphoreType.DMA((chips, 2, 2)),
            pltpu.SemaphoreType.DMA((2, n_dev)),
        ]
        return pl.pallas_call(
            functools.partial(block_kernel, (n_dev, n_seq, n_res, ch, heads)),
            out_shape=jax.ShapeDtypeStruct((n_dev * n_seq, blk, ch), BF16),
            in_specs=[pl.BlockSpec(memory_space=pl.ANY)] * len(args),
            out_specs=pl.BlockSpec(memory_space=pl.ANY),
            scratch_shapes=scratch,
            name="msa_block",
            compiler_params=pltpu.CompilerParams(collective_id=0, has_side_effects=True, vmem_limit_bytes=60 * 2 ** 20),
        )(*args)

    rows_spec = P(('batch', 'seq'))
    return jax.shard_map(local_block, mesh=mesh, in_specs=(rows_spec, rows_spec, rows_spec, P(), P(), P(), P(), P(), P(), P()), out_specs=P('batch', 'seq'), check_vma=False)
```

```python
import functools

import jax
import jax.numpy as jnp
from jax import lax
from jax.experimental import pallas as pl
from jax.experimental.pallas import tpu as pltpu
from jax.sharding import PartitionSpec as P

MESH = pl.DeviceIdType.MESH
LN_EPS = 1.0e-5
MASK_BIG = 1.0e9
MEAN_EPS = 1.0e-10
LOG2E = 1.4426950408889634
EXCLUDED = -3.0e38
F32 = jnp.float32
BF16 = jnp.bfloat16
NT = (((1,), (1,)), ((), ()))


def layer_norm(x_in):
    x = x_in.astype(F32)
    centered = x - jnp.mean(x, axis=-1, keepdims=True)
    var = jnp.mean(centered * centered, axis=-1, keepdims=True)
    return (centered * lax.rsqrt(var + LN_EPS)).astype(BF16)


def dot(a, b):
    return jnp.dot(a, b, preferred_element_type=F32)


def dot_nt(a, b):
    return lax.dot_general(a, b, NT, preferred_element_type=F32)


def iota(shape, dim):
    return lax.broadcasted_iota(jnp.int32, shape, dim)


def block_kernel(dims, e_hbm, m_hbm, z_hbm, wpb_hbm, wri_hbm, wro_hbm, wci_hbm, wco_hbm, wti_hbm, wto_hbm, out_ref,
                 e_v, m_v, z_v, wpb_v, wri_v, wro_v, wci_v, wco_v, wti_v, wto_v,
                 bias32, bias_all, q_s, k_s, v_s, g_s, mb_s, hm_s, bias_t, gt_s, e1_send, e1_recv,
                 wc_s, mrow_s, qsum_s, kt_s, vt_s, gc_s, x_s, p3_s, co_s,
                 in_sem, chain_sem, pair_sem, bias_sem, send_sem, recv_sem):
    n_dev, n_seq, n_res, ch, heads = dims
    chips = n_dev // 2
    reach = chips // 2
    blk = n_res // n_dev
    hd = ch // heads
    c2 = hd ** -0.5 * LOG2E
    hrows = heads * blk
    half = blk // 2
    prows = n_seq * half
    me = lax.axis_index("seq")
    z, c = lax.div(me, 2), lax.rem(me, 2)

    def chip_at(offset):
        return lax.rem(z + offset + chips, chips)

    def slot_of(chip, core):
        return chip * 2 + core

    loads = [(z_hbm, z_v), (wpb_hbm, wpb_v), (e_hbm, e_v), (m_hbm, m_v), (wri_hbm, wri_v), (wro_hbm, wro_v),
             (wci_hbm, wci_v), (wco_hbm, wco_v), (wti_hbm, wti_v), (wto_hbm, wto_v)]
    copies = [pltpu.make_async_copy(src, dst, in_sem.at[n]) for n, (src, dst) in enumerate(loads)]
    for copy in copies:
        copy.start()

    barrier = pltpu.get_barrier_semaphore()
    for d in range(1, n_dev):
        pl.semaphore_signal(barrier, inc=1, device_id={"seq": lax.rem(me + d, n_dev)}, device_id_type=MESH)

    copies[0].wait()
    copies[1].wait()
    wpb_t = wpb_v[...]
    ones = jnp.ones((z_v.shape[2], z_v.shape[2]), BF16)

    def bias_row(i, carry):
        z_row = z_v[i]
        centered = z_row.astype(F32) - dot(z_row, ones) * (1.0 / z_row.shape[1])
        var = jnp.mean(centered * centered, axis=-1, keepdims=True)
        rows = dot_nt(wpb_t, (centered * lax.rsqrt(var + LN_EPS)).astype(BF16))
        for n in range(n_res // 128):
            bias32[n, pl.ds(i, heads, stride=blk), :] = rows[:, n * 128:(n + 1) * 128]
        return carry

    lax.fori_loop(0, blk, bias_row, 0, unroll=True)
    bias_all[me, :hrows] = jnp.concatenate([bias32[n] for n in range(n_res // 128)], axis=-1).astype(BF16)
    copies[3].wait()
    m_f32 = m_v[...].astype(F32)
    mb_s[...] = (MASK_BIG * LOG2E) * (m_f32 - 1.0)
    bias_all[me, hrows:] = jnp.concatenate([m_f32, m_f32], axis=0).astype(BF16)
    pl.semaphore_wait(barrier, n_dev - 1)

    def bias_copy(slot, sem, chip, core, part):
        rows = pl.ds(0, hrows // 2) if part == 0 else pl.ds(hrows // 2, hrows // 2 + 2 * n_seq)
        return pltpu.make_async_remote_copy(
            src_ref=bias_all.at[slot, rows], dst_ref=bias_all.at[slot, rows], send_sem=sem.at[part],
            recv_sem=bias_sem.at[slot, part], device_id={"seq": slot_of(chip, core)}, device_id_type=MESH)

    def up(k, part):
        return bias_copy(slot_of(chip_at(-k), c), chain_sem.at[0, k], chip_at(1), c, part)

    def down(k, part):
        return bias_copy(slot_of(chip_at(k), c), chain_sem.at[1, k], chip_at(-1), c, part)

    def across(offset, t, part):
        return bias_copy(slot_of(chip_at(offset), c), pair_sem.at[t], z, 1 - c, part)

    def bias_wait(offset, core, part):
        bias_copy(slot_of(chip_at(offset), core), pair_sem.at[0], z, c, part).wait_recv()

    for part in range(2):
        up(0, part).start()
        down(0, part).start()
    for part in range(2):
        across(0, 0, part).start()

    for h in range(heads):
        hm_s[h] = jnp.where(lax.div(iota((blk, ch), 1), hd) == h, 1.0, 0.0).astype(BF16)
    copies[2].wait()
    copies[4].wait()

    def project(s, carry):
        proj = dot(layer_norm(e_v[s]), wri_v[...]).astype(BF16)
        q_s[s] = proj[:, :ch]
        k_s[s] = proj[:, ch:2 * ch]
        v_s[s] = proj[:, 2 * ch:3 * ch]
        g_s[s] = proj[:, 3 * ch:]
        return carry

    lax.fori_loop(0, n_seq, project, 0, unroll=True)
    copies[5].wait()

    lane_head = lax.div(iota((blk, ch), 1), hd)

    def own_head(blocks):
        picked = blocks[0]
        for h in range(1, heads):
            picked = jnp.where(lane_head == h, blocks[h], picked)
        return picked

    def e1_copy(t, core, hf):
        return pltpu.make_async_remote_copy(
            src_ref=e1_send.at[t, hf, core], dst_ref=e1_recv.at[hf, me], send_sem=send_sem.at[t, hf, core],
            recv_sem=recv_sem.at[hf, me], device_id={"seq": slot_of(tile_chip(t), core)}, device_id_type=MESH)

    def tile_offset(t):
        k = lax.div(t + 1, 2)
        return k * (2 * lax.rem(t, 2) - 1)

    def tile_chip(t):
        return chip_at(tile_offset(t))

    def send(t, hf):
        for core in range(2):
            e1_copy(t, core, hf).start()

    def row_tile(t, carry):
        k = lax.div(t, 2) + 1

        @pl.when(lax.rem(t, 2) == 0)
        def _():
            for part in range(2):
                bias_wait(-k, c, part)

                @pl.when(k < reach)
                def _():
                    up(k, part).start()

                across(-k, 2 * k - 1, part).start()

                @pl.when(k < reach)
                def _():
                    bias_wait(k, c, part)

                @pl.when(k < reach - 1)
                def _():
                    down(k, part).start()

                @pl.when(k < reach)
                def _():
                    across(k, 2 * k, part).start()

            @pl.when(t == 2)
            def _():
                send(1, 0)

            @pl.when(t == 4)
            def _():
                send(3, 0)
                send(1, 1)
                send(2, 1)

        bias_wait(tile_offset(t), 1 - c, 0)
        bias_wait(tile_offset(t), 1 - c, 1)
        chip = tile_chip(t)
        for core in range(2):
            bias_t[core * hrows:(core + 1) * hrows] = bias_all[slot_of(chip, core), :hrows].astype(F32) * LOG2E
        first = pl.multiple_of(chip * (2 * blk), 2 * blk)

        def logits_of(s):
            parts = []
            for core in range(2):
                q_rows = q_s[s, pl.ds(first + core * blk, blk), :]
                parts += [q_rows * hm_s[h] for h in range(heads)]
            return dot_nt(jnp.concatenate(parts, axis=0), k_s[s])

        logits = logits_of(0)
        for s in range(n_seq):
            ahead = logits_of(s + 1) if s + 1 < n_seq else None
            mask_row = mb_s[s:s + 1, :]
            probs = []
            step = hrows // 2
            for r in range(0, 2 * hrows, step):
                x = logits[r:r + step] * c2 + (bias_t[r:r + step] + mask_row)
                p = jnp.exp2(x - jnp.max(x, axis=-1, keepdims=True))
                probs.append((p * (1.0 / jnp.sum(p, axis=-1, keepdims=True))).astype(BF16))
            attended = dot(jnp.concatenate(probs, axis=0), v_s[s])
            for core in range(2):
                o = own_head([attended[core * hrows + h * blk:core * hrows + (h + 1) * blk] for h in range(heads)])
                gate = jax.nn.sigmoid(g_s[s, pl.ds(first + core * blk, blk), :].astype(F32))
                gated = gate * o
                for hf in range(2):
                    gt_s[hf, core, s] = gated[hf * half:(hf + 1) * half]
            logits = ahead
        update = dot(gt_s[...].reshape(4 * prows, ch).astype(BF16), wro_v[...])
        for core in range(2):
            e_rows = e_v[:, pl.ds(first + core * blk, blk), :].astype(F32)
            for hf in range(2):
                r = (hf * 2 + core) * prows
                e_half = e_rows[:, hf * half:(hf + 1) * half, :].reshape(prows, ch)
                e1_send[t, hf, core] = (e_half + update[r:r + prows]).astype(BF16)

        @pl.when(t == 0)
        def _():
            for hf in range(2):
                e1_recv[hf, me] = e1_send[0, hf, c]
                e1_copy(0, 1 - c, hf).start()

        @pl.when(jnp.logical_or(t == 2, t > 3))
        def _():
            send(t, 0)

        return carry

    lax.fori_loop(0, chips, row_tile, 0)
    for t in range(3, chips):
        send(t, 1)

    copies[6].wait()
    w_k, w_v = wci_v[ch:ch + hd], wci_v[ch + hd:ch + 2 * hd]
    w_all = jnp.concatenate([wci_v[:ch]] + [w_k] * heads + [w_v] * heads + [wci_v[ch + 2 * hd:]], axis=0)
    eye = jnp.where(iota((ch, ch), 0) == iota((ch, ch), 1), 1.0, 0.0).astype(BF16)
    wc_s[...] = dot_nt(eye, w_all).astype(BF16)

    pad = 2 * n_seq
    m_all = bias_all[:, hrows:, :].reshape(n_dev * pad, n_res)
    lane = iota((n_res, 2 * prows), 1)
    row = iota((n_dev * pad, 2 * prows), 0)
    col = iota((n_dev * pad, 2 * prows), 1)
    own = jnp.logical_and(lax.rem(row, pad) == lax.div(lax.rem(col, prows), half), lax.rem(lax.div(row, pad), 2) == lax.div(col, prows))
    for hf in range(2):
        pick = jnp.where(iota((n_res, 2 * prows), 0) == me * blk + hf * half + lax.rem(lane, half), 1.0, 0.0).astype(BF16)
        m_sel = jnp.where(own, dot(m_all, pick), 0.0)
        mrow_s[hf] = jnp.sum(m_sel.reshape(chips, 2 * pad, 2 * prows), axis=1)
    qsum_s[...] = jnp.zeros_like(qsum_s)
    width = 4 * prows
    same = lax.rem(iota((half, width), 1), half) == iota((half, width), 0)
    same_h = lax.rem(iota((heads * half, width), 1), half) == lax.rem(iota((heads * half, width), 0), half)

    def lane_mask(hf, chip_a, chip_b):
        return jnp.concatenate([mrow_s[hf, pl.ds(chip, 1), :] for chip in (chip_a, chip_b)], axis=1)

    def column_in(hf, j):
        sources = [chip_at(-tile_offset(t)) for t in (2 * j, 2 * j + 1)]

        def arrival(chip, core):
            slot = slot_of(chip, core)
            pltpu.make_async_remote_copy(
                src_ref=e1_send.at[0, 0, 0], dst_ref=e1_recv.at[hf, slot], send_sem=send_sem.at[0, 0, 0],
                recv_sem=recv_sem.at[hf, slot], device_id={"seq": me}, device_id_type=MESH).wait_recv()

        if j == 0:
            arrival(sources[0], 1 - c)
        else:
            arrival(sources[0], 0)
            arrival(sources[0], 1)
        arrival(sources[1], 0)
        arrival(sources[1], 1)
        rows = jnp.concatenate([e1_recv[hf, pl.ds(chip * 2, 2)].reshape(2 * prows, ch) for chip in sources], axis=0)
        proj = dot(layer_norm(rows), wc_s[...]).astype(BF16)
        for n, chip in enumerate(sources):
            part = proj[n * 2 * prows:(n + 1) * 2 * prows]
            kt_s[hf, chip] = part[:, ch:2 * ch]
            vt_s[hf, chip] = part[:, 2 * ch:3 * ch]
            gc_s[hf, chip] = part[:, 3 * ch:]
        sel = jnp.where(same, lane_mask(hf, sources[0], sources[1]), 0.0).astype(BF16)
        qsum_s[hf] += dot(sel, proj[:, :ch])

    def column_attention(hf):
        count = jnp.sum(mrow_s[hf], axis=0, keepdims=True)
        count = jnp.sum(jnp.where(same[:, :2 * prows], count, 0.0), axis=-1, keepdims=True)
        q_mean = (qsum_s[hf] / (count + MEAN_EPS)).astype(BF16).astype(F32)
        q_rows = jnp.concatenate([q_mean * hm_s[h, :half].astype(F32) for h in range(heads)], axis=0).astype(BF16)
        n_rows = heads * half
        top = jnp.full((n_rows, width), EXCLUDED, F32)
        for pair in range(chips // 2):
            keys = kt_s[hf, 2 * pair:2 * pair + 2].reshape(width, ch)
            x = dot_nt(q_rows, keys) * c2 + (MASK_BIG * LOG2E) * (lane_mask(hf, 2 * pair, 2 * pair + 1) - 1.0)
            x = jnp.where(same_h, x, EXCLUDED)
            x_s[pair] = x
            top = jnp.maximum(top, x)
        top = jnp.max(top, axis=-1, keepdims=True)
        total = jnp.zeros((n_rows, width), F32)
        for pair in range(chips // 2):
            p = jnp.exp2(x_s[pair] - top)
            total = total + p
            for n in range(3):
                piece = p.astype(BF16)
                p3_s[n * n_rows:(n + 1) * n_rows, pair * width:(pair + 1) * width] = piece
                p = p - piece.astype(F32)
        o3 = dot(p3_s[...], vt_s[hf].reshape(chips * 2 * prows, ch))
        o = (o3[:n_rows] + o3[n_rows:2 * n_rows] + o3[2 * n_rows:]) / jnp.sum(total, axis=-1, keepdims=True)
        head = lane_head[:half]
        picked = o[:half]
        for h in range(1, heads):
            picked = jnp.where(head == h, o[h * half:(h + 1) * half], picked)
        co_s[...] = picked

    n_out = 4 * n_seq

    def finish_pair(hf, pair):
        e1 = e1_recv[hf, pl.ds(pair * 4, 4)].reshape(width, ch).astype(F32)
        gate = jax.nn.sigmoid(gc_s[hf, pl.ds(pair * 2, 2)].reshape(width, ch).astype(F32)).reshape(n_out, half, ch)
        gated = (gate * co_s[...][None]).reshape(width, ch).astype(BF16)
        e2 = (e1 + dot(gated, wco_v[...])).astype(BF16)
        hidden = jnp.maximum(dot(layer_norm(e2), wti_v[...]), 0.0).astype(BF16)
        e3 = e2.astype(F32) + dot(hidden, wto_v[...])
        out_ref[pair * n_out:(pair + 1) * n_out, hf * half:(hf + 1) * half, :] = e3.reshape(n_out, half, ch).astype(BF16)

    def finish(hf):
        for pair in range(chips // 2):
            finish_pair(hf, pair)

    column_in(0, 0)
    column_in(0, 1)
    column_in(0, 2)
    column_in(0, 3)
    column_attention(0)
    copies[7].wait()
    copies[8].wait()
    copies[9].wait()
    finish(0)
    for j in range(chips // 2):
        column_in(1, j)
    column_attention(1)
    finish(1)

    for part in range(2):
        for k in range(reach):
            up(k, part).wait_send()
            if k < reach - 1:
                down(k, part).wait_send()
        for t in range(chips):
            across(0, t, part).wait_send()
    for hf in range(2):
        e1_copy(0, 1 - c, hf).wait_send()
        for core in range(2):
            for t in range(1, chips):
                e1_copy(t, core, hf).wait_send()


def solution(mesh):
    n_dev = mesh.shape["seq"]

    def local_block(e, m, z, w_pair_bias, w_row_in, w_row_out, w_col_in, w_col_out, w_trans_in, w_trans_out):
        n_seq, n_res, ch = e.shape
        heads = w_pair_bias.shape[1]
        blk = n_res // n_dev
        chips = n_dev // 2
        half = blk // 2
        hrows, prows = heads * blk, n_seq * half
        args = (e, m, z, w_pair_bias.T, w_row_in, w_row_out, w_col_in.T, w_col_out, w_trans_in, w_trans_out)
        scratch = [pltpu.VMEM(a.shape, a.dtype) for a in args] + [
            pltpu.VMEM((n_res // 128, hrows, 128), F32),
            pltpu.VMEM((n_dev, hrows + 2 * n_seq, n_res), BF16),
            pltpu.VMEM((n_seq, n_res, ch), BF16),
            pltpu.VMEM((n_seq, n_res, ch), BF16),
            pltpu.VMEM((n_seq, n_res, ch), BF16),
            pltpu.VMEM((n_seq, n_res, ch), BF16),
            pltpu.VMEM((n_seq, n_res), F32),
            pltpu.VMEM((heads, blk, ch), BF16),
            pltpu.VMEM((2 * hrows, n_res), F32),
            pltpu.VMEM((2, 2, n_seq, half, ch), F32),
            pltpu.VMEM((chips, 2, 2, prows, ch), BF16),
            pltpu.VMEM((2, n_dev, prows, ch), BF16),
            pltpu.VMEM((ch, 4 * ch), BF16),
            pltpu.VMEM((2, chips, 2 * prows), F32),
            pltpu.VMEM((2, half, ch), F32),
            pltpu.VMEM((2, chips, 2 * prows, ch), BF16),
            pltpu.VMEM((2, chips, 2 * prows, ch), BF16),
            pltpu.VMEM((2, chips, 2 * prows, ch), BF16),
            pltpu.VMEM((chips // 2, heads * half, 4 * prows), F32),
            pltpu.VMEM((3 * heads * half, n_dev * prows), BF16),
            pltpu.VMEM((half, ch), F32),
            pltpu.SemaphoreType.DMA((len(args),)),
            pltpu.SemaphoreType.DMA((2, chips // 2, 2)),
            pltpu.SemaphoreType.DMA((chips, 2)),
            pltpu.SemaphoreType.DMA((n_dev, 2)),
            pltpu.SemaphoreType.DMA((chips, 2, 2)),
            pltpu.SemaphoreType.DMA((2, n_dev)),
        ]
        return pl.pallas_call(
            functools.partial(block_kernel, (n_dev, n_seq, n_res, ch, heads)),
            out_shape=pltpu.VMEM((n_dev * n_seq, blk, ch), BF16),
            in_specs=[pl.BlockSpec(memory_space=pl.ANY)] * len(args),
            out_specs=pl.BlockSpec(memory_space=pltpu.VMEM),
            scratch_shapes=scratch,
            name="msa_block",
            compiler_params=pltpu.CompilerParams(collective_id=0, has_side_effects=True, vmem_limit_bytes=60 * 2 ** 20),
        )(*args)

    rows_spec = P(('batch', 'seq'))
    return jax.shard_map(local_block, mesh=mesh, in_specs=(rows_spec, rows_spec, rows_spec, P(), P(), P(), P(), P(), P(), P()), out_specs=P('batch', 'seq'), check_vma=False)
```

```python
import functools

import jax
import jax.numpy as jnp
from jax import lax
from jax.experimental import pallas as pl
from jax.experimental.pallas import tpu as pltpu
from jax.sharding import PartitionSpec as P

MESH = pl.DeviceIdType.MESH
LN_EPS = 1.0e-5
MASK_BIG = 1.0e9
MEAN_EPS = 1.0e-10
LOG2E = 1.4426950408889634
EXCLUDED = -3.0e38
F32 = jnp.float32
BF16 = jnp.bfloat16
NT = (((1,), (1,)), ((), ()))


def layer_norm(x_in):
    x = x_in.astype(F32)
    centered = x - jnp.mean(x, axis=-1, keepdims=True)
    var = jnp.mean(centered * centered, axis=-1, keepdims=True)
    return (centered * lax.rsqrt(var + LN_EPS)).astype(BF16)


def dot(a, b):
    return jnp.dot(a, b, preferred_element_type=F32)


def dot_nt(a, b):
    return lax.dot_general(a, b, NT, preferred_element_type=F32)


def iota(shape, dim):
    return lax.broadcasted_iota(jnp.int32, shape, dim)


def block_kernel(dims, e_hbm, m_hbm, z_hbm, wpb_hbm, wri_hbm, wro_hbm, wci_hbm, wco_hbm, wti_hbm, wto_hbm, out_ref,
                 e_v, m_v, z_v, wpb_v, wri_v, wro_v, wci_v, wco_v, wti_v, wto_v,
                 bias32, bias_all, q_s, k_s, v_s, g_s, mb_s, hm_s, bias_t, gt_s, e1_send, e1_recv,
                 wc_s, mrow_s, qsum_s, kt_s, vt_s, gc_s, x_s, p3_s, co_s,
                 in_sem, chain_sem, pair_sem, bias_sem, send_sem, recv_sem):
    n_dev, n_seq, n_res, ch, heads = dims
    chips = n_dev // 2
    reach = chips // 2
    blk = n_res // n_dev
    hd = ch // heads
    c2 = hd ** -0.5 * LOG2E
    hrows = heads * blk
    half = blk // 2
    prows = n_seq * half
    me = lax.axis_index("seq")
    z, c = lax.div(me, 2), lax.rem(me, 2)

    def chip_at(offset):
        return lax.rem(z + offset + chips, chips)

    def slot_of(chip, core):
        return chip * 2 + core

    loads = [(z_hbm, z_v), (wpb_hbm, wpb_v), (e_hbm, e_v), (m_hbm, m_v), (wri_hbm, wri_v), (wro_hbm, wro_v),
             (wci_hbm, wci_v), (wco_hbm, wco_v), (wti_hbm, wti_v), (wto_hbm, wto_v)]
    copies = [pltpu.make_async_copy(src, dst, in_sem.at[n]) for n, (src, dst) in enumerate(loads)]
    for copy in copies:
        copy.start()

    barrier = pltpu.get_barrier_semaphore()
    for d in range(1, n_dev):
        pl.semaphore_signal(barrier, inc=1, device_id={"seq": lax.rem(me + d, n_dev)}, device_id_type=MESH)

    copies[0].wait()
    copies[1].wait()
    wpb_t = wpb_v[...]
    ones = jnp.ones((z_v.shape[2], z_v.shape[2]), BF16)

    def bias_row(i, carry):
        z_row = z_v[i]
        centered = z_row.astype(F32) - dot(z_row, ones) * (1.0 / z_row.shape[1])
        var = jnp.mean(centered * centered, axis=-1, keepdims=True)
        rows = dot_nt(wpb_t, (centered * lax.rsqrt(var + LN_EPS)).astype(BF16))
        for n in range(n_res // 128):
            bias32[n, pl.ds(i, heads, stride=blk), :] = rows[:, n * 128:(n + 1) * 128]
        return carry

    lax.fori_loop(0, blk, bias_row, 0, unroll=True)
    bias_all[me, :hrows] = jnp.concatenate([bias32[n] for n in range(n_res // 128)], axis=-1).astype(BF16)
    copies[3].wait()
    m_f32 = m_v[...].astype(F32)
    mb_s[...] = (MASK_BIG * LOG2E) * (m_f32 - 1.0)
    bias_all[me, hrows:] = jnp.concatenate([m_f32, m_f32], axis=0).astype(BF16)
    pl.semaphore_wait(barrier, n_dev - 1)

    def bias_copy(slot, sem, chip, core, part):
        rows = pl.ds(0, hrows // 2) if part == 0 else pl.ds(hrows // 2, hrows // 2 + 2 * n_seq)
        return pltpu.make_async_remote_copy(
            src_ref=bias_all.at[slot, rows], dst_ref=bias_all.at[slot, rows], send_sem=sem.at[part],
            recv_sem=bias_sem.at[slot, part], device_id={"seq": slot_of(chip, core)}, device_id_type=MESH)

    def up(k, part):
        return bias_copy(slot_of(chip_at(-k), c), chain_sem.at[0, k], chip_at(1), c, part)

    def down(k, part):
        return bias_copy(slot_of(chip_at(k), c), chain_sem.at[1, k], chip_at(-1), c, part)

    def across(offset, t, part):
        return bias_copy(slot_of(chip_at(offset), c), pair_sem.at[t], z, 1 - c, part)

    def bias_wait(offset, core, part):
        bias_copy(slot_of(chip_at(offset), core), pair_sem.at[0], z, c, part).wait_recv()

    for part in range(2):
        up(0, part).start()
        down(0, part).start()
    for part in range(2):
        across(0, 0, part).start()

    for h in range(heads):
        hm_s[h] = jnp.where(lax.div(iota((blk, ch), 1), hd) == h, 1.0, 0.0).astype(BF16)
    copies[2].wait()
    copies[4].wait()

    def project(s, carry):
        proj = dot(layer_norm(e_v[s]), wri_v[...]).astype(BF16)
        q_s[s] = proj[:, :ch]
        k_s[s] = proj[:, ch:2 * ch]
        v_s[s] = proj[:, 2 * ch:3 * ch]
        g_s[s] = proj[:, 3 * ch:]
        return carry

    lax.fori_loop(0, n_seq, project, 0, unroll=True)
    copies[5].wait()

    lane_head = lax.div(iota((blk, ch), 1), hd)

    def own_head(blocks):
        picked = blocks[0]
        for h in range(1, heads):
            picked = jnp.where(lane_head == h, blocks[h], picked)
        return picked

    def e1_copy(t, core, hf):
        return pltpu.make_async_remote_copy(
            src_ref=e1_send.at[t, hf, core], dst_ref=e1_recv.at[hf, me], send_sem=send_sem.at[t, hf, core],
            recv_sem=recv_sem.at[hf, me], device_id={"seq": slot_of(tile_chip(t), core)}, device_id_type=MESH)

    def tile_offset(t):
        k = lax.div(t + 1, 2)
        return k * (2 * lax.rem(t, 2) - 1)

    def tile_chip(t):
        return chip_at(tile_offset(t))

    def send(t, hf):
        for core in range(2):
            e1_copy(t, core, hf).start()

    def row_tile(t, carry):
        k = lax.div(t, 2) + 1

        @pl.when(lax.rem(t, 2) == 0)
        def _():
            for part in range(2):
                bias_wait(-k, c, part)

                @pl.when(k < reach)
                def _():
                    up(k, part).start()

                across(-k, 2 * k - 1, part).start()

                @pl.when(k < reach)
                def _():
                    bias_wait(k, c, part)

                @pl.when(k < reach - 1)
                def _():
                    down(k, part).start()

                @pl.when(k < reach)
                def _():
                    across(k, 2 * k, part).start()

            @pl.when(t == 2)
            def _():
                send(1, 0)
                send(1, 1)

            @pl.when(t == 4)
            def _():
                send(3, 0)

        bias_wait(tile_offset(t), 1 - c, 0)
        bias_wait(tile_offset(t), 1 - c, 1)
        chip = tile_chip(t)
        for core in range(2):
            bias_t[core * hrows:(core + 1) * hrows] = bias_all[slot_of(chip, core), :hrows].astype(F32) * LOG2E
        first = pl.multiple_of(chip * (2 * blk), 2 * blk)

        def logits_of(s):
            parts = []
            for core in range(2):
                q_rows = q_s[s, pl.ds(first + core * blk, blk), :]
                parts += [q_rows * hm_s[h] for h in range(heads)]
            return dot_nt(jnp.concatenate(parts, axis=0), k_s[s])

        logits = logits_of(0)
        for s in range(n_seq):
            ahead = logits_of(s + 1) if s + 1 < n_seq else None
            mask_row = mb_s[s:s + 1, :]
            probs = []
            step = hrows // 2
            for r in range(0, 2 * hrows, step):
                x = logits[r:r + step] * c2 + (bias_t[r:r + step] + mask_row)
                p = jnp.exp2(x - jnp.max(x, axis=-1, keepdims=True))
                probs.append((p * (1.0 / jnp.sum(p, axis=-1, keepdims=True))).astype(BF16))
            attended = dot(jnp.concatenate(probs, axis=0), v_s[s])
            for core in range(2):
                o = own_head([attended[core * hrows + h * blk:core * hrows + (h + 1) * blk] for h in range(heads)])
                gate = jax.nn.sigmoid(g_s[s, pl.ds(first + core * blk, blk), :].astype(F32))
                gated = gate * o
                for hf in range(2):
                    gt_s[hf, core, s] = gated[hf * half:(hf + 1) * half]
            logits = ahead
        update = dot(gt_s[...].reshape(4 * prows, ch).astype(BF16), wro_v[...])
        for core in range(2):
            e_rows = e_v[:, pl.ds(first + core * blk, blk), :].astype(F32)
            for hf in range(2):
                r = (hf * 2 + core) * prows
                e_half = e_rows[:, hf * half:(hf + 1) * half, :].reshape(prows, ch)
                e1_send[t, hf, core] = (e_half + update[r:r + prows]).astype(BF16)

        @pl.when(t == 0)
        def _():
            for hf in range(2):
                e1_recv[hf, me] = e1_send[0, hf, c]
                e1_copy(0, 1 - c, hf).start()

        @pl.when(jnp.logical_or(t == 2, t > 3))
        def _():
            send(t, 0)

        @pl.when(t == 2)
        def _():
            send(2, 1)

        return carry

    lax.fori_loop(0, chips, row_tile, 0)
    for t in range(3, chips):
        send(t, 1)

    copies[6].wait()
    w_k, w_v = wci_v[ch:ch + hd], wci_v[ch + hd:ch + 2 * hd]
    w_all = jnp.concatenate([wci_v[:ch]] + [w_k] * heads + [w_v] * heads + [wci_v[ch + 2 * hd:]], axis=0)
    eye = jnp.where(iota((ch, ch), 0) == iota((ch, ch), 1), 1.0, 0.0).astype(BF16)
    wc_s[...] = dot_nt(eye, w_all).astype(BF16)

    pad = 2 * n_seq
    m_all = bias_all[:, hrows:, :].reshape(n_dev * pad, n_res)
    lane = iota((n_res, 2 * prows), 1)
    row = iota((n_dev * pad, 2 * prows), 0)
    col = iota((n_dev * pad, 2 * prows), 1)
    own = jnp.logical_and(lax.rem(row, pad) == lax.div(lax.rem(col, prows), half), lax.rem(lax.div(row, pad), 2) == lax.div(col, prows))
    for hf in range(2):
        pick = jnp.where(iota((n_res, 2 * prows), 0) == me * blk + hf * half + lax.rem(lane, half), 1.0, 0.0).astype(BF16)
        m_sel = jnp.where(own, dot(m_all, pick), 0.0)
        mrow_s[hf] = jnp.sum(m_sel.reshape(chips, 2 * pad, 2 * prows), axis=1)
    qsum_s[...] = jnp.zeros_like(qsum_s)
    width = 4 * prows
    same = lax.rem(iota((half, width), 1), half) == iota((half, width), 0)
    same_h = lax.rem(iota((heads * half, width), 1), half) == lax.rem(iota((heads * half, width), 0), half)

    def lane_mask(hf, chip_a, chip_b):
        return jnp.concatenate([mrow_s[hf, pl.ds(chip, 1), :] for chip in (chip_a, chip_b)], axis=1)

    def column_in(hf, j):
        sources = [chip_at(-tile_offset(t)) for t in (2 * j, 2 * j + 1)]

        def arrival(chip, core):
            slot = slot_of(chip, core)
            pltpu.make_async_remote_copy(
                src_ref=e1_send.at[0, 0, 0], dst_ref=e1_recv.at[hf, slot], send_sem=send_sem.at[0, 0, 0],
                recv_sem=recv_sem.at[hf, slot], device_id={"seq": me}, device_id_type=MESH).wait_recv()

        if j == 0:
            arrival(sources[0], 1 - c)
        else:
            arrival(sources[0], 0)
            arrival(sources[0], 1)
        arrival(sources[1], 0)
        arrival(sources[1], 1)
        rows = jnp.concatenate([e1_recv[hf, pl.ds(chip * 2, 2)].reshape(2 * prows, ch) for chip in sources], axis=0)
        proj = dot(layer_norm(rows), wc_s[...]).astype(BF16)
        for n, chip in enumerate(sources):
            part = proj[n * 2 * prows:(n + 1) * 2 * prows]
            kt_s[hf, chip] = part[:, ch:2 * ch]
            vt_s[hf, chip] = part[:, 2 * ch:3 * ch]
            gc_s[hf, chip] = part[:, 3 * ch:]
        sel = jnp.where(same, lane_mask(hf, sources[0], sources[1]), 0.0).astype(BF16)
        qsum_s[hf] += dot(sel, proj[:, :ch])

    def column_attention(hf):
        count = jnp.sum(mrow_s[hf], axis=0, keepdims=True)
        count = jnp.sum(jnp.where(same[:, :2 * prows], count, 0.0), axis=-1, keepdims=True)
        q_mean = (qsum_s[hf] / (count + MEAN_EPS)).astype(BF16).astype(F32)
        q_rows = jnp.concatenate([q_mean * hm_s[h, :half].astype(F32) for h in range(heads)], axis=0).astype(BF16)
        n_rows = heads * half
        top = jnp.full((n_rows, width), EXCLUDED, F32)
        for pair in range(chips // 2):
            keys = kt_s[hf, 2 * pair:2 * pair + 2].reshape(width, ch)
            x = dot_nt(q_rows, keys) * c2 + (MASK_BIG * LOG2E) * (lane_mask(hf, 2 * pair, 2 * pair + 1) - 1.0)
            x = jnp.where(same_h, x, EXCLUDED)
            x_s[pair] = x
            top = jnp.maximum(top, x)
        top = jnp.max(top, axis=-1, keepdims=True)
        total = jnp.zeros((n_rows, width), F32)
        for pair in range(chips // 2):
            p = jnp.exp2(x_s[pair] - top)
            total = total + p
            for n in range(3):
                piece = p.astype(BF16)
                p3_s[n * n_rows:(n + 1) * n_rows, pair * width:(pair + 1) * width] = piece
                p = p - piece.astype(F32)
        o3 = dot(p3_s[...], vt_s[hf].reshape(chips * 2 * prows, ch))
        o = (o3[:n_rows] + o3[n_rows:2 * n_rows] + o3[2 * n_rows:]) / jnp.sum(total, axis=-1, keepdims=True)
        head = lane_head[:half]
        picked = o[:half]
        for h in range(1, heads):
            picked = jnp.where(head == h, o[h * half:(h + 1) * half], picked)
        co_s[...] = picked

    n_out = 4 * n_seq

    def finish_pair(hf, pair):
        e1 = e1_recv[hf, pl.ds(pair * 4, 4)].reshape(width, ch).astype(F32)
        gate = jax.nn.sigmoid(gc_s[hf, pl.ds(pair * 2, 2)].reshape(width, ch).astype(F32)).reshape(n_out, half, ch)
        gated = (gate * co_s[...][None]).reshape(width, ch).astype(BF16)
        e2 = (e1 + dot(gated, wco_v[...])).astype(BF16)
        hidden = jnp.maximum(dot(layer_norm(e2), wti_v[...]), 0.0).astype(BF16)
        e3 = e2.astype(F32) + dot(hidden, wto_v[...])
        out_ref[pair * n_out:(pair + 1) * n_out, hf * half:(hf + 1) * half, :] = e3.reshape(n_out, half, ch).astype(BF16)

    def finish(hf):
        for pair in range(chips // 2):
            finish_pair(hf, pair)

    column_in(0, 0)
    column_in(0, 1)
    column_in(0, 2)
    column_in(0, 3)
    column_attention(0)
    copies[7].wait()
    copies[8].wait()
    copies[9].wait()
    finish(0)
    for j in range(chips // 2):
        column_in(1, j)
    column_attention(1)
    finish(1)

    for part in range(2):
        for k in range(reach):
            up(k, part).wait_send()
            if k < reach - 1:
                down(k, part).wait_send()
        for t in range(chips):
            across(0, t, part).wait_send()
    for hf in range(2):
        e1_copy(0, 1 - c, hf).wait_send()
        for core in range(2):
            for t in range(1, chips):
                e1_copy(t, core, hf).wait_send()


def solution(mesh):
    n_dev = mesh.shape["seq"]

    def local_block(e, m, z, w_pair_bias, w_row_in, w_row_out, w_col_in, w_col_out, w_trans_in, w_trans_out):
        n_seq, n_res, ch = e.shape
        heads = w_pair_bias.shape[1]
        blk = n_res // n_dev
        chips = n_dev // 2
        half = blk // 2
        hrows, prows = heads * blk, n_seq * half
        args = (e, m, z, w_pair_bias.T, w_row_in, w_row_out, w_col_in.T, w_col_out, w_trans_in, w_trans_out)
        scratch = [pltpu.VMEM(a.shape, a.dtype) for a in args] + [
            pltpu.VMEM((n_res // 128, hrows, 128), F32),
            pltpu.VMEM((n_dev, hrows + 2 * n_seq, n_res), BF16),
            pltpu.VMEM((n_seq, n_res, ch), BF16),
            pltpu.VMEM((n_seq, n_res, ch), BF16),
            pltpu.VMEM((n_seq, n_res, ch), BF16),
            pltpu.VMEM((n_seq, n_res, ch), BF16),
            pltpu.VMEM((n_seq, n_res), F32),
            pltpu.VMEM((heads, blk, ch), BF16),
            pltpu.VMEM((2 * hrows, n_res), F32),
            pltpu.VMEM((2, 2, n_seq, half, ch), F32),
            pltpu.VMEM((chips, 2, 2, prows, ch), BF16),
            pltpu.VMEM((2, n_dev, prows, ch), BF16),
            pltpu.VMEM((ch, 4 * ch), BF16),
            pltpu.VMEM((2, chips, 2 * prows), F32),
            pltpu.VMEM((2, half, ch), F32),
            pltpu.VMEM((2, chips, 2 * prows, ch), BF16),
            pltpu.VMEM((2, chips, 2 * prows, ch), BF16),
            pltpu.VMEM((2, chips, 2 * prows, ch), BF16),
            pltpu.VMEM((chips // 2, heads * half, 4 * prows), F32),
            pltpu.VMEM((3 * heads * half, n_dev * prows), BF16),
            pltpu.VMEM((half, ch), F32),
            pltpu.SemaphoreType.DMA((len(args),)),
            pltpu.SemaphoreType.DMA((2, chips // 2, 2)),
            pltpu.SemaphoreType.DMA((chips, 2)),
            pltpu.SemaphoreType.DMA((n_dev, 2)),
            pltpu.SemaphoreType.DMA((chips, 2, 2)),
            pltpu.SemaphoreType.DMA((2, n_dev)),
        ]
        return pl.pallas_call(
            functools.partial(block_kernel, (n_dev, n_seq, n_res, ch, heads)),
            out_shape=pltpu.VMEM((n_dev * n_seq, blk, ch), BF16),
            in_specs=[pl.BlockSpec(memory_space=pl.ANY)] * len(args),
            out_specs=pl.BlockSpec(memory_space=pltpu.VMEM),
            scratch_shapes=scratch,
            name="msa_block",
            compiler_params=pltpu.CompilerParams(collective_id=0, has_side_effects=True, vmem_limit_bytes=60 * 2 ** 20),
        )(*args)

    rows_spec = P(('batch', 'seq'))
    return jax.shard_map(local_block, mesh=mesh, in_specs=(rows_spec, rows_spec, rows_spec, P(), P(), P(), P(), P(), P(), P()), out_specs=P('batch', 'seq'), check_vma=False)
```

```python
import functools

import jax
import jax.numpy as jnp
from jax import lax
from jax.experimental import pallas as pl
from jax.experimental.pallas import tpu as pltpu
from jax.sharding import PartitionSpec as P

MESH = pl.DeviceIdType.MESH
LN_EPS = 1.0e-5
MASK_BIG = 1.0e9
MEAN_EPS = 1.0e-10
LOG2E = 1.4426950408889634
EXCLUDED = -3.0e38
F32 = jnp.float32
BF16 = jnp.bfloat16
NT = (((1,), (1,)), ((), ()))


def layer_norm(x_in):
    x = x_in.astype(F32)
    centered = x - jnp.mean(x, axis=-1, keepdims=True)
    var = jnp.mean(centered * centered, axis=-1, keepdims=True)
    return (centered * lax.rsqrt(var + LN_EPS)).astype(BF16)


def dot(a, b):
    return jnp.dot(a, b, preferred_element_type=F32)


def dot_nt(a, b):
    return lax.dot_general(a, b, NT, preferred_element_type=F32)


def iota(shape, dim):
    return lax.broadcasted_iota(jnp.int32, shape, dim)


def block_kernel(dims, e_hbm, m_hbm, z_hbm, wpb_hbm, wri_hbm, wro_hbm, wci_hbm, wco_hbm, wti_hbm, wto_hbm, out_ref,
                 e_v, m_v, z_v, wpb_v, wri_v, wro_v, wci_v, wco_v, wti_v, wto_v,
                 bias32, bias_all, q_s, k_s, v_s, g_s, mb_s, hm_s, bias_t, gt_s, e1_send, e1_recv,
                 wc_s, mrow_s, qsum_s, kt_s, vt_s, gc_s, x_s, p3_s, co_s,
                 in_sem, chain_sem, pair_sem, bias_sem, send_sem, recv_sem):
    n_dev, n_seq, n_res, ch, heads = dims
    chips = n_dev // 2
    reach = chips // 2
    blk = n_res // n_dev
    hd = ch // heads
    c2 = hd ** -0.5 * LOG2E
    hrows = heads * blk
    half = blk // 2
    prows = n_seq * half
    me = lax.axis_index("seq")
    z, c = lax.div(me, 2), lax.rem(me, 2)

    def chip_at(offset):
        return lax.rem(z + offset + chips, chips)

    def slot_of(chip, core):
        return chip * 2 + core

    loads = [(z_hbm, z_v), (wpb_hbm, wpb_v), (e_hbm, e_v), (m_hbm, m_v), (wri_hbm, wri_v), (wro_hbm, wro_v),
             (wci_hbm, wci_v), (wco_hbm, wco_v), (wti_hbm, wti_v), (wto_hbm, wto_v)]
    copies = [pltpu.make_async_copy(src, dst, in_sem.at[n]) for n, (src, dst) in enumerate(loads)]
    copies[0].start()
    copies[1].start()

    barrier = pltpu.get_barrier_semaphore()
    for d in range(1, n_dev):
        pl.semaphore_signal(barrier, inc=1, device_id={"seq": lax.rem(me + d, n_dev)}, device_id_type=MESH)

    copies[0].wait()
    copies[1].wait()
    for copy in copies[2:]:
        copy.start()
    wpb_t = wpb_v[...]
    ones = jnp.ones((z_v.shape[2], z_v.shape[2]), BF16)

    def bias_row(i, carry):
        z_row = z_v[i]
        centered = z_row.astype(F32) - dot(z_row, ones) * (1.0 / z_row.shape[1])
        var = jnp.mean(centered * centered, axis=-1, keepdims=True)
        rows = dot_nt(wpb_t, (centered * lax.rsqrt(var + LN_EPS)).astype(BF16))
        for n in range(n_res // 128):
            bias32[n, pl.ds(i, heads, stride=blk), :] = rows[:, n * 128:(n + 1) * 128]
        return carry

    lax.fori_loop(0, blk, bias_row, 0, unroll=True)
    bias_all[me, :hrows] = jnp.concatenate([bias32[n] for n in range(n_res // 128)], axis=-1).astype(BF16)
    copies[3].wait()
    m_f32 = m_v[...].astype(F32)
    mb_s[...] = (MASK_BIG * LOG2E) * (m_f32 - 1.0)
    bias_all[me, hrows:] = jnp.concatenate([m_f32, m_f32], axis=0).astype(BF16)
    pl.semaphore_wait(barrier, n_dev - 1)

    def bias_copy(slot, sem, chip, core, part):
        rows = pl.ds(0, hrows // 2) if part == 0 else pl.ds(hrows // 2, hrows // 2 + 2 * n_seq)
        return pltpu.make_async_remote_copy(
            src_ref=bias_all.at[slot, rows], dst_ref=bias_all.at[slot, rows], send_sem=sem.at[part],
            recv_sem=bias_sem.at[slot, part], device_id={"seq": slot_of(chip, core)}, device_id_type=MESH)

    def up(k, part):
        return bias_copy(slot_of(chip_at(-k), c), chain_sem.at[0, k], chip_at(1), c, part)

    def down(k, part):
        return bias_copy(slot_of(chip_at(k), c), chain_sem.at[1, k], chip_at(-1), c, part)

    def across(offset, t, part):
        return bias_copy(slot_of(chip_at(offset), c), pair_sem.at[t], z, 1 - c, part)

    def bias_wait(offset, core, part):
        bias_copy(slot_of(chip_at(offset), core), pair_sem.at[0], z, c, part).wait_recv()

    for part in range(2):
        up(0, part).start()
        down(0, part).start()
    for part in range(2):
        across(0, 0, part).start()

    for h in range(heads):
        hm_s[h] = jnp.where(lax.div(iota((blk, ch), 1), hd) == h, 1.0, 0.0).astype(BF16)
    copies[2].wait()
    copies[4].wait()

    def project(s, carry):
        proj = dot(layer_norm(e_v[s]), wri_v[...]).astype(BF16)
        q_s[s] = proj[:, :ch]
        k_s[s] = proj[:, ch:2 * ch]
        v_s[s] = proj[:, 2 * ch:3 * ch]
        g_s[s] = proj[:, 3 * ch:]
        return carry

    lax.fori_loop(0, n_seq, project, 0, unroll=True)
    copies[5].wait()

    lane_head = lax.div(iota((blk, ch), 1), hd)

    def own_head(blocks):
        picked = blocks[0]
        for h in range(1, heads):
            picked = jnp.where(lane_head == h, blocks[h], picked)
        return picked

    def e1_copy(t, core, hf):
        return pltpu.make_async_remote_copy(
            src_ref=e1_send.at[t, hf, core], dst_ref=e1_recv.at[hf, me], send_sem=send_sem.at[t, hf, core],
            recv_sem=recv_sem.at[hf, me], device_id={"seq": slot_of(tile_chip(t), core)}, device_id_type=MESH)

    def tile_offset(t):
        k = lax.div(t + 1, 2)
        return k * (2 * lax.rem(t, 2) - 1)

    def tile_chip(t):
        return chip_at(tile_offset(t))

    def send(t, hf):
        for core in range(2):
            e1_copy(t, core, hf).start()

    def row_tile(t, carry):
        k = lax.div(t, 2) + 1

        @pl.when(lax.rem(t, 2) == 0)
        def _():
            for part in range(2):
                bias_wait(-k, c, part)

                @pl.when(k < reach)
                def _():
                    up(k, part).start()

                across(-k, 2 * k - 1, part).start()

                @pl.when(k < reach)
                def _():
                    bias_wait(k, c, part)

                @pl.when(k < reach - 1)
                def _():
                    down(k, part).start()

                @pl.when(k < reach)
                def _():
                    across(k, 2 * k, part).start()

            @pl.when(t == 2)
            def _():
                send(1, 0)
                send(1, 1)

            @pl.when(t == 4)
            def _():
                send(3, 0)

        bias_wait(tile_offset(t), 1 - c, 0)
        bias_wait(tile_offset(t), 1 - c, 1)
        chip = tile_chip(t)
        for core in range(2):
            bias_t[core * hrows:(core + 1) * hrows] = bias_all[slot_of(chip, core), :hrows].astype(F32) * LOG2E
        first = pl.multiple_of(chip * (2 * blk), 2 * blk)

        def logits_of(s):
            parts = []
            for core in range(2):
                q_rows = q_s[s, pl.ds(first + core * blk, blk), :]
                parts += [q_rows * hm_s[h] for h in range(heads)]
            return dot_nt(jnp.concatenate(parts, axis=0), k_s[s])

        logits = logits_of(0)
        for s in range(n_seq):
            ahead = logits_of(s + 1) if s + 1 < n_seq else None
            mask_row = mb_s[s:s + 1, :]
            probs = []
            step = hrows // 2
            for r in range(0, 2 * hrows, step):
                x = logits[r:r + step] * c2 + (bias_t[r:r + step] + mask_row)
                p = jnp.exp2(x - jnp.max(x, axis=-1, keepdims=True))
                probs.append((p * (1.0 / jnp.sum(p, axis=-1, keepdims=True))).astype(BF16))
            attended = dot(jnp.concatenate(probs, axis=0), v_s[s])
            for core in range(2):
                o = own_head([attended[core * hrows + h * blk:core * hrows + (h + 1) * blk] for h in range(heads)])
                gate = jax.nn.sigmoid(g_s[s, pl.ds(first + core * blk, blk), :].astype(F32))
                gated = gate * o
                for hf in range(2):
                    gt_s[hf, core, s] = gated[hf * half:(hf + 1) * half]
            logits = ahead
        update = dot(gt_s[...].reshape(4 * prows, ch).astype(BF16), wro_v[...])
        for core in range(2):
            e_rows = e_v[:, pl.ds(first + core * blk, blk), :].astype(F32)
            for hf in range(2):
                r = (hf * 2 + core) * prows
                e_half = e_rows[:, hf * half:(hf + 1) * half, :].reshape(prows, ch)
                e1_send[t, hf, core] = (e_half + update[r:r + prows]).astype(BF16)

        @pl.when(t == 0)
        def _():
            for hf in range(2):
                e1_recv[hf, me] = e1_send[0, hf, c]
                e1_copy(0, 1 - c, hf).start()

        @pl.when(jnp.logical_or(t == 2, t > 3))
        def _():
            send(t, 0)

        @pl.when(t == 2)
        def _():
            send(2, 1)

        return carry

    lax.fori_loop(0, chips, row_tile, 0)
    for t in [chips - 1] + list(range(chips - 3, chips - 1)) + list(range(3, chips - 3)):
        send(t, 1)

    copies[6].wait()
    w_k, w_v = wci_v[ch:ch + hd], wci_v[ch + hd:ch + 2 * hd]
    w_all = jnp.concatenate([wci_v[:ch]] + [w_k] * heads + [w_v] * heads + [wci_v[ch + 2 * hd:]], axis=0)
    eye = jnp.where(iota((ch, ch), 0) == iota((ch, ch), 1), 1.0, 0.0).astype(BF16)
    wc_s[...] = dot_nt(eye, w_all).astype(BF16)

    pad = 2 * n_seq
    m_all = bias_all[:, hrows:, :].reshape(n_dev * pad, n_res)
    lane = iota((n_res, 2 * prows), 1)
    row = iota((n_dev * pad, 2 * prows), 0)
    col = iota((n_dev * pad, 2 * prows), 1)
    own = jnp.logical_and(lax.rem(row, pad) == lax.div(lax.rem(col, prows), half), lax.rem(lax.div(row, pad), 2) == lax.div(col, prows))
    for hf in range(2):
        pick = jnp.where(iota((n_res, 2 * prows), 0) == me * blk + hf * half + lax.rem(lane, half), 1.0, 0.0).astype(BF16)
        m_sel = jnp.where(own, dot(m_all, pick), 0.0)
        mrow_s[hf] = jnp.sum(m_sel.reshape(chips, 2 * pad, 2 * prows), axis=1)
    qsum_s[...] = jnp.zeros_like(qsum_s)
    width = 4 * prows
    same = lax.rem(iota((half, width), 1), half) == iota((half, width), 0)
    same_h = lax.rem(iota((heads * half, width), 1), half) == lax.rem(iota((heads * half, width), 0), half)

    def lane_mask(hf, chip_a, chip_b):
        return jnp.concatenate([mrow_s[hf, pl.ds(chip, 1), :] for chip in (chip_a, chip_b)], axis=1)

    def column_in(hf, j):
        sources = [chip_at(-tile_offset(t)) for t in (2 * j, 2 * j + 1)]

        def arrival(chip, core):
            slot = slot_of(chip, core)
            pltpu.make_async_remote_copy(
                src_ref=e1_send.at[0, 0, 0], dst_ref=e1_recv.at[hf, slot], send_sem=send_sem.at[0, 0, 0],
                recv_sem=recv_sem.at[hf, slot], device_id={"seq": me}, device_id_type=MESH).wait_recv()

        if j == 0:
            arrival(sources[0], 1 - c)
        else:
            arrival(sources[0], 0)
            arrival(sources[0], 1)
        arrival(sources[1], 0)
        arrival(sources[1], 1)
        rows = jnp.concatenate([e1_recv[hf, pl.ds(chip * 2, 2)].reshape(2 * prows, ch) for chip in sources], axis=0)
        proj = dot(layer_norm(rows), wc_s[...]).astype(BF16)
        for n, chip in enumerate(sources):
            part = proj[n * 2 * prows:(n + 1) * 2 * prows]
            kt_s[hf, chip] = part[:, ch:2 * ch]
            vt_s[hf, chip] = part[:, 2 * ch:3 * ch]
            gc_s[hf, chip] = part[:, 3 * ch:]
        sel = jnp.where(same, lane_mask(hf, sources[0], sources[1]), 0.0).astype(BF16)
        qsum_s[hf] += dot(sel, proj[:, :ch])

    def column_attention(hf):
        count = jnp.sum(mrow_s[hf], axis=0, keepdims=True)
        count = jnp.sum(jnp.where(same[:, :2 * prows], count, 0.0), axis=-1, keepdims=True)
        q_mean = (qsum_s[hf] / (count + MEAN_EPS)).astype(BF16).astype(F32)
        q_rows = jnp.concatenate([q_mean * hm_s[h, :half].astype(F32) for h in range(heads)], axis=0).astype(BF16)
        n_rows = heads * half
        top = jnp.full((n_rows, width), EXCLUDED, F32)
        for pair in range(chips // 2):
            keys = kt_s[hf, 2 * pair:2 * pair + 2].reshape(width, ch)
            x = dot_nt(q_rows, keys) * c2 + (MASK_BIG * LOG2E) * (lane_mask(hf, 2 * pair, 2 * pair + 1) - 1.0)
            x = jnp.where(same_h, x, EXCLUDED)
            x_s[pair] = x
            top = jnp.maximum(top, x)
        top = jnp.max(top, axis=-1, keepdims=True)
        total = jnp.zeros((n_rows, width), F32)
        for pair in range(chips // 2):
            p = jnp.exp2(x_s[pair] - top)
            total = total + p
            for n in range(3):
                piece = p.astype(BF16)
                p3_s[n * n_rows:(n + 1) * n_rows, pair * width:(pair + 1) * width] = piece
                p = p - piece.astype(F32)
        o3 = dot(p3_s[...], vt_s[hf].reshape(chips * 2 * prows, ch))
        o = (o3[:n_rows] + o3[n_rows:2 * n_rows] + o3[2 * n_rows:]) / jnp.sum(total, axis=-1, keepdims=True)
        head = lane_head[:half]
        picked = o[:half]
        for h in range(1, heads):
            picked = jnp.where(head == h, o[h * half:(h + 1) * half], picked)
        co_s[...] = picked

    n_out = 4 * n_seq

    def finish_pair(hf, pair):
        e1 = e1_recv[hf, pl.ds(pair * 4, 4)].reshape(width, ch).astype(F32)
        gate = jax.nn.sigmoid(gc_s[hf, pl.ds(pair * 2, 2)].reshape(width, ch).astype(F32)).reshape(n_out, half, ch)
        gated = (gate * co_s[...][None]).reshape(width, ch).astype(BF16)
        e2 = (e1 + dot(gated, wco_v[...])).astype(BF16)
        hidden = jnp.maximum(dot(layer_norm(e2), wti_v[...]), 0.0).astype(BF16)
        e3 = e2.astype(F32) + dot(hidden, wto_v[...])
        out_ref[pair * n_out:(pair + 1) * n_out, hf * half:(hf + 1) * half, :] = e3.reshape(n_out, half, ch).astype(BF16)

    def finish(hf):
        for pair in range(chips // 2):
            finish_pair(hf, pair)

    column_in(0, 0)
    column_in(0, 1)
    column_in(0, 2)
    column_in(0, 3)
    column_attention(0)
    copies[7].wait()
    copies[8].wait()
    copies[9].wait()
    finish(0)
    for j in [0] + list(range(chips // 2 - 1, 0, -1)):
        column_in(1, j)
    column_attention(1)
    finish(1)

    for part in range(2):
        for k in range(reach):
            up(k, part).wait_send()
            if k < reach - 1:
                down(k, part).wait_send()
        for t in range(chips):
            across(0, t, part).wait_send()
    for hf in range(2):
        e1_copy(0, 1 - c, hf).wait_send()
        for core in range(2):
            for t in range(1, chips):
                e1_copy(t, core, hf).wait_send()


def solution(mesh):
    n_dev = mesh.shape["seq"]

    def local_block(e, m, z, w_pair_bias, w_row_in, w_row_out, w_col_in, w_col_out, w_trans_in, w_trans_out):
        n_seq, n_res, ch = e.shape
        heads = w_pair_bias.shape[1]
        blk = n_res // n_dev
        chips = n_dev // 2
        half = blk // 2
        hrows, prows = heads * blk, n_seq * half
        args = (e, m, z, w_pair_bias.T, w_row_in, w_row_out, w_col_in.T, w_col_out, w_trans_in, w_trans_out)
        scratch = [pltpu.VMEM(a.shape, a.dtype) for a in args] + [
            pltpu.VMEM((n_res // 128, hrows, 128), F32),
            pltpu.VMEM((n_dev, hrows + 2 * n_seq, n_res), BF16),
            pltpu.VMEM((n_seq, n_res, ch), BF16),
            pltpu.VMEM((n_seq, n_res, ch), BF16),
            pltpu.VMEM((n_seq, n_res, ch), BF16),
            pltpu.VMEM((n_seq, n_res, ch), BF16),
            pltpu.VMEM((n_seq, n_res), F32),
            pltpu.VMEM((heads, blk, ch), BF16),
            pltpu.VMEM((2 * hrows, n_res), F32),
            pltpu.VMEM((2, 2, n_seq, half, ch), F32),
            pltpu.VMEM((chips, 2, 2, prows, ch), BF16),
            pltpu.VMEM((2, n_dev, prows, ch), BF16),
            pltpu.VMEM((ch, 4 * ch), BF16),
            pltpu.VMEM((2, chips, 2 * prows), F32),
            pltpu.VMEM((2, half, ch), F32),
            pltpu.VMEM((2, chips, 2 * prows, ch), BF16),
            pltpu.VMEM((2, chips, 2 * prows, ch), BF16),
            pltpu.VMEM((2, chips, 2 * prows, ch), BF16),
            pltpu.VMEM((chips // 2, heads * half, 4 * prows), F32),
            pltpu.VMEM((3 * heads * half, n_dev * prows), BF16),
            pltpu.VMEM((half, ch), F32),
            pltpu.SemaphoreType.DMA((len(args),)),
            pltpu.SemaphoreType.DMA((2, chips // 2, 2)),
            pltpu.SemaphoreType.DMA((chips, 2)),
            pltpu.SemaphoreType.DMA((n_dev, 2)),
            pltpu.SemaphoreType.DMA((chips, 2, 2)),
            pltpu.SemaphoreType.DMA((2, n_dev)),
        ]
        return pl.pallas_call(
            functools.partial(block_kernel, (n_dev, n_seq, n_res, ch, heads)),
            out_shape=pltpu.VMEM((n_dev * n_seq, blk, ch), BF16),
            in_specs=[pl.BlockSpec(memory_space=pl.ANY)] * len(args),
            out_specs=pl.BlockSpec(memory_space=pltpu.VMEM),
            scratch_shapes=scratch,
            name="msa_block",
            compiler_params=pltpu.CompilerParams(collective_id=0, has_side_effects=True, vmem_limit_bytes=60 * 2 ** 20),
        )(*args)

    rows_spec = P(('batch', 'seq'))
    return jax.shard_map(local_block, mesh=mesh, in_specs=(rows_spec, rows_spec, rows_spec, P(), P(), P(), P(), P(), P(), P()), out_specs=P('batch', 'seq'), check_vma=False)
```

```python
import functools

import jax
import jax.numpy as jnp
from jax import lax
from jax.experimental import pallas as pl
from jax.experimental.pallas import tpu as pltpu
from jax.sharding import PartitionSpec as P

MESH = pl.DeviceIdType.MESH
LN_EPS = 1.0e-5
MASK_BIG = 1.0e9
MEAN_EPS = 1.0e-10
LOG2E = 1.4426950408889634
EXCLUDED = -3.0e38
F32 = jnp.float32
BF16 = jnp.bfloat16
NT = (((1,), (1,)), ((), ()))


def layer_norm(x_in):
    x = x_in.astype(F32)
    centered = x - jnp.mean(x, axis=-1, keepdims=True)
    var = jnp.mean(centered * centered, axis=-1, keepdims=True)
    return (centered * lax.rsqrt(var + LN_EPS)).astype(BF16)


def dot(a, b):
    return jnp.dot(a, b, preferred_element_type=F32)


def dot_nt(a, b):
    return lax.dot_general(a, b, NT, preferred_element_type=F32)


def iota(shape, dim):
    return lax.broadcasted_iota(jnp.int32, shape, dim)


def block_kernel(dims, e_hbm, m_hbm, z_hbm, wpb_hbm, wri_hbm, wro_hbm, wci_hbm, wco_hbm, wti_hbm, wto_hbm, out_ref,
                 e_v, m_v, z_v, wpb_v, wri_v, wro_v, wci_v, wco_v, wti_v, wto_v,
                 bias32, bias_all, q_s, k_s, v_s, g_s, mb_s, hm_s, bias_t, gt_s, e1_send, e1_recv,
                 wc_s, mrow_s, qsum_s, kt_s, vt_s, gc_s, x_s, p3_s, co_s,
                 in_sem, chain_sem, pair_sem, bias_sem, send_sem, recv_sem):
    n_dev, n_seq, n_res, ch, heads = dims
    chips = n_dev // 2
    reach = chips // 2
    blk = n_res // n_dev
    hd = ch // heads
    c2 = hd ** -0.5 * LOG2E
    hrows = heads * blk
    half = blk // 2
    prows = n_seq * half
    me = lax.axis_index("seq")
    z, c = lax.div(me, 2), lax.rem(me, 2)

    def chip_at(offset):
        return lax.rem(z + offset + chips, chips)

    def slot_of(chip, core):
        return chip * 2 + core

    loads = [(z_hbm, z_v), (wpb_hbm, wpb_v), (e_hbm, e_v), (m_hbm, m_v), (wri_hbm, wri_v), (wro_hbm, wro_v),
             (wci_hbm, wci_v), (wco_hbm, wco_v), (wti_hbm, wti_v), (wto_hbm, wto_v)]
    copies = [pltpu.make_async_copy(src, dst, in_sem.at[n]) for n, (src, dst) in enumerate(loads)]
    copies[0].start()
    copies[1].start()

    barrier = pltpu.get_barrier_semaphore()
    for d in range(1, n_dev):
        pl.semaphore_signal(barrier, inc=1, device_id={"seq": lax.rem(me + d, n_dev)}, device_id_type=MESH)

    copies[0].wait()
    copies[1].wait()
    for copy in copies[2:]:
        copy.start()
    wpb_t = wpb_v[...]
    ones = jnp.ones((z_v.shape[2], z_v.shape[2]), BF16)

    def bias_row(i, carry):
        z_row = z_v[i]
        centered = z_row.astype(F32) - dot(z_row, ones) * (1.0 / z_row.shape[1])
        var = jnp.mean(centered * centered, axis=-1, keepdims=True)
        rows = dot_nt(wpb_t, (centered * lax.rsqrt(var + LN_EPS)).astype(BF16))
        for n in range(n_res // 128):
            bias32[n, pl.ds(i, heads, stride=blk), :] = rows[:, n * 128:(n + 1) * 128]
        return carry

    lax.fori_loop(0, blk, bias_row, 0, unroll=True)
    bias_all[me, :hrows] = jnp.concatenate([bias32[n] for n in range(n_res // 128)], axis=-1).astype(BF16)
    copies[3].wait()
    m_f32 = m_v[...].astype(F32)
    mb_s[...] = (MASK_BIG * LOG2E) * (m_f32 - 1.0)
    bias_all[me, hrows:] = jnp.concatenate([m_f32, m_f32], axis=0).astype(BF16)
    pl.semaphore_wait(barrier, n_dev - 1)

    def bias_copy(slot, sem, chip, core, part):
        rows = pl.ds(0, hrows // 2) if part == 0 else pl.ds(hrows // 2, hrows // 2 + 2 * n_seq)
        return pltpu.make_async_remote_copy(
            src_ref=bias_all.at[slot, rows], dst_ref=bias_all.at[slot, rows], send_sem=sem.at[part],
            recv_sem=bias_sem.at[slot, part], device_id={"seq": slot_of(chip, core)}, device_id_type=MESH)

    def up(k, part):
        return bias_copy(slot_of(chip_at(-k), c), chain_sem.at[0, k], chip_at(1), c, part)

    def down(k, part):
        return bias_copy(slot_of(chip_at(k), c), chain_sem.at[1, k], chip_at(-1), c, part)

    def across(offset, t, part):
        return bias_copy(slot_of(chip_at(offset), c), pair_sem.at[t], z, 1 - c, part)

    def bias_wait(offset, core, part):
        bias_copy(slot_of(chip_at(offset), core), pair_sem.at[0], z, c, part).wait_recv()

    for part in range(2):
        up(0, part).start()
        down(0, part).start()
    for part in range(2):
        across(0, 0, part).start()

    for h in range(heads):
        hm_s[h] = jnp.where(lax.div(iota((blk, ch), 1), hd) == h, 1.0, 0.0).astype(BF16)
    copies[2].wait()
    copies[4].wait()

    def project(s, carry):
        proj = dot(layer_norm(e_v[s]), wri_v[...]).astype(BF16)
        q_s[s] = proj[:, :ch]
        k_s[s] = proj[:, ch:2 * ch]
        v_s[s] = proj[:, 2 * ch:3 * ch]
        g_s[s] = proj[:, 3 * ch:]
        return carry

    lax.fori_loop(0, n_seq, project, 0, unroll=True)
    copies[5].wait()

    lane_head = lax.div(iota((blk, ch), 1), hd)

    def own_head(blocks):
        picked = blocks[0]
        for h in range(1, heads):
            picked = jnp.where(lane_head == h, blocks[h], picked)
        return picked

    def e1_copy(t, core, hf):
        return pltpu.make_async_remote_copy(
            src_ref=e1_send.at[t, hf, core], dst_ref=e1_recv.at[hf, me], send_sem=send_sem.at[t, hf, core],
            recv_sem=recv_sem.at[hf, me], device_id={"seq": slot_of(tile_chip(t), core)}, device_id_type=MESH)

    def tile_offset(t):
        k = lax.div(t + 1, 2)
        return k * (2 * lax.rem(t, 2) - 1)

    def tile_chip(t):
        return chip_at(tile_offset(t))

    def send(t, hf):
        for core in range(2):
            e1_copy(t, core, hf).start()

    def row_tile(t, carry):
        k = lax.div(t, 2) + 1

        @pl.when(lax.rem(t, 2) == 0)
        def _():
            for part in range(2):
                bias_wait(-k, c, part)

                @pl.when(k < reach)
                def _():
                    up(k, part).start()

                across(-k, 2 * k - 1, part).start()

                @pl.when(k < reach)
                def _():
                    bias_wait(k, c, part)

                @pl.when(k < reach - 1)
                def _():
                    down(k, part).start()

                @pl.when(k < reach)
                def _():
                    across(k, 2 * k, part).start()

            @pl.when(t == 2)
            def _():
                send(1, 0)
                send(1, 1)

            @pl.when(t == 4)
            def _():
                send(3, 0)

        bias_wait(tile_offset(t), 1 - c, 0)
        bias_wait(tile_offset(t), 1 - c, 1)
        chip = tile_chip(t)
        for core in range(2):
            bias_t[core * hrows:(core + 1) * hrows] = bias_all[slot_of(chip, core), :hrows].astype(F32) * LOG2E
        first = pl.multiple_of(chip * (2 * blk), 2 * blk)

        def logits_of(s):
            parts = []
            for core in range(2):
                q_rows = q_s[s, pl.ds(first + core * blk, blk), :]
                parts += [q_rows * hm_s[h] for h in range(heads)]
            return dot_nt(jnp.concatenate(parts, axis=0), k_s[s])

        logits = logits_of(0)
        for s in range(n_seq):
            ahead = logits_of(s + 1) if s + 1 < n_seq else None
            mask_row = mb_s[s:s + 1, :]
            probs = []
            step = hrows // 2
            for r in range(0, 2 * hrows, step):
                x = logits[r:r + step] * c2 + (bias_t[r:r + step] + mask_row)
                p = jnp.exp2(x - jnp.max(x, axis=-1, keepdims=True))
                probs.append((p * (1.0 / jnp.sum(p, axis=-1, keepdims=True))).astype(BF16))
            attended = dot(jnp.concatenate(probs, axis=0), v_s[s])
            for core in range(2):
                o = own_head([attended[core * hrows + h * blk:core * hrows + (h + 1) * blk] for h in range(heads)])
                gate = jax.nn.sigmoid(g_s[s, pl.ds(first + core * blk, blk), :].astype(F32))
                gated = gate * o
                for hf in range(2):
                    gt_s[hf, core, s] = gated[hf * half:(hf + 1) * half]
            logits = ahead
        update = dot(gt_s[...].reshape(4 * prows, ch).astype(BF16), wro_v[...])
        for core in range(2):
            e_rows = e_v[:, pl.ds(first + core * blk, blk), :].astype(F32)
            for hf in range(2):
                r = (hf * 2 + core) * prows
                e_half = e_rows[:, hf * half:(hf + 1) * half, :].reshape(prows, ch)
                e1_send[t, hf, core] = (e_half + update[r:r + prows]).astype(BF16)

        @pl.when(t == 0)
        def _():
            for hf in range(2):
                e1_recv[hf, me] = e1_send[0, hf, c]
                e1_copy(0, 1 - c, hf).start()

        @pl.when(jnp.logical_or(t == 2, t > 3))
        def _():
            send(t, 0)

        @pl.when(t == 2)
        def _():
            send(2, 1)

        return carry

    lax.fori_loop(0, chips, row_tile, 0)
    for t in range(3, chips):
        send(t, 1)

    copies[6].wait()
    w_k, w_v = wci_v[ch:ch + hd], wci_v[ch + hd:ch + 2 * hd]
    w_all = jnp.concatenate([wci_v[:ch]] + [w_k] * heads + [w_v] * heads + [wci_v[ch + 2 * hd:]], axis=0)
    eye = jnp.where(iota((ch, ch), 0) == iota((ch, ch), 1), 1.0, 0.0).astype(BF16)
    wc_s[...] = dot_nt(eye, w_all).astype(BF16)

    pad = 2 * n_seq
    m_all = bias_all[:, hrows:, :].reshape(n_dev * pad, n_res)
    lane = iota((n_res, 2 * prows), 1)
    row = iota((n_dev * pad, 2 * prows), 0)
    col = iota((n_dev * pad, 2 * prows), 1)
    own = jnp.logical_and(lax.rem(row, pad) == lax.div(lax.rem(col, prows), half), lax.rem(lax.div(row, pad), 2) == lax.div(col, prows))
    for hf in range(2):
        pick = jnp.where(iota((n_res, 2 * prows), 0) == me * blk + hf * half + lax.rem(lane, half), 1.0, 0.0).astype(BF16)
        m_sel = jnp.where(own, dot(m_all, pick), 0.0)
        mrow_s[hf] = jnp.sum(m_sel.reshape(chips, 2 * pad, 2 * prows), axis=1)
    qsum_s[...] = jnp.zeros_like(qsum_s)
    width = 4 * prows
    same = lax.rem(iota((half, width), 1), half) == iota((half, width), 0)
    same_h = lax.rem(iota((heads * half, width), 1), half) == lax.rem(iota((heads * half, width), 0), half)

    def lane_mask(hf, chip_a, chip_b):
        return jnp.concatenate([mrow_s[hf, pl.ds(chip, 1), :] for chip in (chip_a, chip_b)], axis=1)

    def column_in(hf, j):
        sources = [chip_at(-tile_offset(t)) for t in (2 * j, 2 * j + 1)]

        def arrival(chip, core):
            slot = slot_of(chip, core)
            pltpu.make_async_remote_copy(
                src_ref=e1_send.at[0, 0, 0], dst_ref=e1_recv.at[hf, slot], send_sem=send_sem.at[0, 0, 0],
                recv_sem=recv_sem.at[hf, slot], device_id={"seq": me}, device_id_type=MESH).wait_recv()

        if j == 0:
            arrival(sources[0], 1 - c)
        else:
            arrival(sources[0], 0)
            arrival(sources[0], 1)
        arrival(sources[1], 0)
        arrival(sources[1], 1)
        rows = jnp.concatenate([e1_recv[hf, pl.ds(chip * 2, 2)].reshape(2 * prows, ch) for chip in sources], axis=0)
        proj = dot(layer_norm(rows), wc_s[...]).astype(BF16)
        for n, chip in enumerate(sources):
            part = proj[n * 2 * prows:(n + 1) * 2 * prows]
            kt_s[hf, chip] = part[:, ch:2 * ch]
            vt_s[hf, chip] = part[:, 2 * ch:3 * ch]
            gc_s[hf, chip] = part[:, 3 * ch:]
        sel = jnp.where(same, lane_mask(hf, sources[0], sources[1]), 0.0).astype(BF16)
        qsum_s[hf] += dot(sel, proj[:, :ch])

    def column_attention(hf):
        count = jnp.sum(mrow_s[hf], axis=0, keepdims=True)
        count = jnp.sum(jnp.where(same[:, :2 * prows], count, 0.0), axis=-1, keepdims=True)
        q_mean = (qsum_s[hf] / (count + MEAN_EPS)).astype(BF16).astype(F32)
        q_rows = jnp.concatenate([q_mean * hm_s[h, :half].astype(F32) for h in range(heads)], axis=0).astype(BF16)
        n_rows = heads * half
        top = jnp.full((n_rows, width), EXCLUDED, F32)
        for pair in range(chips // 2):
            keys = kt_s[hf, 2 * pair:2 * pair + 2].reshape(width, ch)
            x = dot_nt(q_rows, keys) * c2 + (MASK_BIG * LOG2E) * (lane_mask(hf, 2 * pair, 2 * pair + 1) - 1.0)
            x = jnp.where(same_h, x, EXCLUDED)
            x_s[pair] = x
            top = jnp.maximum(top, x)
        top = jnp.max(top, axis=-1, keepdims=True)
        total = jnp.zeros((n_rows, width), F32)
        for pair in range(chips // 2):
            p = jnp.exp2(x_s[pair] - top)
            total = total + p
            for n in range(3):
                piece = p.astype(BF16)
                p3_s[n * n_rows:(n + 1) * n_rows, pair * width:(pair + 1) * width] = piece
                p = p - piece.astype(F32)
        o3 = dot(p3_s[...], vt_s[hf].reshape(chips * 2 * prows, ch))
        o = (o3[:n_rows] + o3[n_rows:2 * n_rows] + o3[2 * n_rows:]) / jnp.sum(total, axis=-1, keepdims=True)
        head = lane_head[:half]
        picked = o[:half]
        for h in range(1, heads):
            picked = jnp.where(head == h, o[h * half:(h + 1) * half], picked)
        co_s[...] = picked

    n_out = 4 * n_seq

    def finish_pair(hf, pair):
        e1 = e1_recv[hf, pl.ds(pair * 4, 4)].reshape(width, ch).astype(F32)
        gate = jax.nn.sigmoid(gc_s[hf, pl.ds(pair * 2, 2)].reshape(width, ch).astype(F32)).reshape(n_out, half, ch)
        gated = (gate * co_s[...][None]).reshape(width, ch).astype(BF16)
        e2 = (e1 + dot(gated, wco_v[...])).astype(BF16)
        hidden = jnp.maximum(dot(layer_norm(e2), wti_v[...]), 0.0).astype(BF16)
        e3 = e2.astype(F32) + dot(hidden, wto_v[...])
        out_ref[pair * n_out:(pair + 1) * n_out, hf * half:(hf + 1) * half, :] = e3.reshape(n_out, half, ch).astype(BF16)

    def finish(hf):
        for pair in range(chips // 2):
            finish_pair(hf, pair)

    column_in(0, 0)
    column_in(0, 1)
    column_in(0, 2)
    column_in(0, 3)
    column_attention(0)
    copies[7].wait()
    copies[8].wait()
    copies[9].wait()
    finish(0)
    for j in range(chips // 2):
        column_in(1, j)
    column_attention(1)
    finish(1)

    for part in range(2):
        for k in range(reach):
            up(k, part).wait_send()
            if k < reach - 1:
                down(k, part).wait_send()
        for t in range(chips):
            across(0, t, part).wait_send()
    for hf in range(2):
        e1_copy(0, 1 - c, hf).wait_send()
        for core in range(2):
            for t in range(1, chips):
                e1_copy(t, core, hf).wait_send()


def solution(mesh):
    n_dev = mesh.shape["seq"]

    def local_block(e, m, z, w_pair_bias, w_row_in, w_row_out, w_col_in, w_col_out, w_trans_in, w_trans_out):
        n_seq, n_res, ch = e.shape
        heads = w_pair_bias.shape[1]
        blk = n_res // n_dev
        chips = n_dev // 2
        half = blk // 2
        hrows, prows = heads * blk, n_seq * half
        args = (e, m, z, w_pair_bias.T, w_row_in, w_row_out, w_col_in.T, w_col_out, w_trans_in, w_trans_out)
        scratch = [pltpu.VMEM(a.shape, a.dtype) for a in args] + [
            pltpu.VMEM((n_res // 128, hrows, 128), F32),
            pltpu.VMEM((n_dev, hrows + 2 * n_seq, n_res), BF16),
            pltpu.VMEM((n_seq, n_res, ch), BF16),
            pltpu.VMEM((n_seq, n_res, ch), BF16),
            pltpu.VMEM((n_seq, n_res, ch), BF16),
            pltpu.VMEM((n_seq, n_res, ch), BF16),
            pltpu.VMEM((n_seq, n_res), F32),
            pltpu.VMEM((heads, blk, ch), BF16),
            pltpu.VMEM((2 * hrows, n_res), F32),
            pltpu.VMEM((2, 2, n_seq, half, ch), F32),
            pltpu.VMEM((chips, 2, 2, prows, ch), BF16),
            pltpu.VMEM((2, n_dev, prows, ch), BF16),
            pltpu.VMEM((ch, 4 * ch), BF16),
            pltpu.VMEM((2, chips, 2 * prows), F32),
            pltpu.VMEM((2, half, ch), F32),
            pltpu.VMEM((2, chips, 2 * prows, ch), BF16),
            pltpu.VMEM((2, chips, 2 * prows, ch), BF16),
            pltpu.VMEM((2, chips, 2 * prows, ch), BF16),
            pltpu.VMEM((chips // 2, heads * half, 4 * prows), F32),
            pltpu.VMEM((3 * heads * half, n_dev * prows), BF16),
            pltpu.VMEM((half, ch), F32),
            pltpu.SemaphoreType.DMA((len(args),)),
            pltpu.SemaphoreType.DMA((2, chips // 2, 2)),
            pltpu.SemaphoreType.DMA((chips, 2)),
            pltpu.SemaphoreType.DMA((n_dev, 2)),
            pltpu.SemaphoreType.DMA((chips, 2, 2)),
            pltpu.SemaphoreType.DMA((2, n_dev)),
        ]
        return pl.pallas_call(
            functools.partial(block_kernel, (n_dev, n_seq, n_res, ch, heads)),
            out_shape=pltpu.VMEM((n_dev * n_seq, blk, ch), BF16),
            in_specs=[pl.BlockSpec(memory_space=pl.ANY)] * len(args),
            out_specs=pl.BlockSpec(memory_space=pltpu.VMEM),
            scratch_shapes=scratch,
            name="msa_block",
            compiler_params=pltpu.CompilerParams(collective_id=0, has_side_effects=True, vmem_limit_bytes=60 * 2 ** 20),
        )(*args)

    rows_spec = P(('batch', 'seq'))
    return jax.shard_map(local_block, mesh=mesh, in_specs=(rows_spec, rows_spec, rows_spec, P(), P(), P(), P(), P(), P(), P()), out_specs=P('batch', 'seq'), check_vma=False)
```
